256 devices in a mesh: win: 128 (over y, x, z), head: 2 (over core).
Axes of the slice: x: 4, y: 4, z: 8, core: 2. Of those that a mesh axis runs over, the one named last changes fastest.
Arguments:
- coords: float32 [3, 4096, 128], P(None, 'win', 'head'), may hold values from -8 to 16
- noise: float32 [3, 4096, 128], P(None, 'win', 'head'), may hold values from -6 to 6
- sigma: float32 [1], replicated, may hold values from 0.25 to 1
- atom_single: bfloat16 [4096, 128, 128], P('win', 'head'), may hold values from -6 to 6
- token_single: bfloat16 [65536, 384], P('win'), may hold values from -6 to 6
- atom_token: int32 [4096, 128], P('win', 'head'), may hold values from 0 to 15, never falling along the last dimension, each value on 1 to 64 neighbouring positions
- window_count: int32 [128], replicated, may hold values from 1 to 31, as said below
- pair_bias: bfloat16 [4, 4096, 128, 128], P('head', 'win'), may hold values from -6 to 260
- token_weight: bfloat16 [384, 128], replicated, may hold values from -0.3125 to 0.3125
- cond_gain: float32 [128], replicated, may hold values from 0.25 to 1.75
- position_weight: float32 [3, 128], replicated, may hold values from -3.5 to 3.5
- ada_weight: bfloat16 [3, 6, 128, 128], replicated, may hold values from -0.5 to 0.5
- ada_bias: float32 [3, 6, 128], replicated, may hold values from -4 to 4
- attn_weight: bfloat16 [3, 4, 128, 128], P(None, None, None, 'head'), may hold values from -0.5 to 0.5
- out_weight: bfloat16 [3, 128, 128], P(None, 'head'), may hold values from -0.5 to 0.5
- gateup_weight: bfloat16 [3, 2, 128, 256], replicated, may hold values from -0.5 to 0.5
- down_weight: bfloat16 [3, 256, 128], replicated, may hold values from -0.375 to 0.375
- final_weight: bfloat16 [3, 128], replicated, may hold values from -0.5 to 0.5
Outputs:
- denoised: float32 [3, 4096, 128], P(None, 'win', 'head')
The draws below stay inside these ranges and needn't reach their ends.
Inputs may be any that keep to these rules, and one draw needn't show every extreme that they name: window_count[d] + window_count[d + 64] <= 32 for every d < 64, with equality for some d.
All inputs are finite; a program needn't handle non-finite values.
Results may differ from the reference program's by a relative error of at most 0.005.
Values may be sent and summed in bfloat16 or wider, within the bound.
A program may use at most 128 MiB of HBM per device.

```python
import math
import jax
import jax.numpy as jnp
import numpy as np
from jax import lax

C = 128
HEADS = 4
HEAD_DIM = 32
HID = 256
C_S = 384
QW = 128
TOKW = 16
BLOCKS = 3
WIN_DEV = 32
TOK_DEV = 512
WINDOWS = 4096
TOKENS = 65536
N_WIN = 128


def draw_coords(key, part):
    first_key = jax.random.fold_in(jax.random.fold_in(key, 11), 0)
    along = jnp.arange(WINDOWS, dtype=jnp.float32) / WINDOWS
    component = (jnp.arange(3) == 0).astype(jnp.float32)
    rough = jnp.clip(jax.random.normal(first_key, (3, WINDOWS, QW), jnp.float32), -4.0, 4.0)
    offset = 2.0 + 4.0 * along
    return rough + component[:, None, None] * offset[None, :, None]


def draw_window_count(key, part):
    half_count = N_WIN // 2
    first_key, second_key, third_key = jax.random.split(jax.random.fold_in(key, 23), 3)
    positions = jnp.arange(half_count, dtype=jnp.int32)
    first_count = jax.random.randint(first_key, (half_count,), 1, WIN_DEV, dtype=jnp.int32)
    first_count = jnp.where(positions == 0, WIN_DEV - 1, first_count)
    room_left = WIN_DEV - first_count
    second_count = 1 + jax.random.randint(second_key, (half_count,), 0, 1048576, dtype=jnp.int32) % room_left
    second_count = jnp.where(positions == 0, room_left, second_count)
    flipped = jax.random.randint(third_key, (half_count,), 0, 2, dtype=jnp.int32)
    lower_half = jnp.where(flipped == 1, second_count, first_count)
    upper_half = jnp.where(flipped == 1, first_count, second_count)
    return jnp.concatenate([lower_half, upper_half]).astype(jnp.int32)


def draw_pair_bias(key, part):
    first_key = jax.random.fold_in(jax.random.fold_in(key, 37), 0)
    shape_all = (HEADS, WINDOWS, QW, QW)
    base = jnp.clip(jax.random.normal(first_key, shape_all, jnp.float32), -6.0, 6.0)
    return base.astype(jnp.bfloat16)


def block_scale(stream_key, dims, shards, smallest, high):
    gain, own = 1.0, jax.random.fold_in(stream_key, 6)
    for dim, blocks in shards:
        heights = jnp.exp(jax.random.uniform(jax.random.fold_in(own, dim), (blocks,), jnp.float32, smallest / len(shards), high / len(shards)))
        gain = gain * jnp.repeat(heights, dims[dim] // blocks).reshape([-1 if axis == dim else 1 for axis in range(len(dims))])
    return gain


def profile(number_of, total, bound, skew):
    portions = [(1 << 20) // math.isqrt(rank ** skew) + 1 for rank in range(2, number_of + 1)]
    rest, given = total - bound - (number_of - 1), [1] * (number_of - 1)
    while rest > 0:
        candidates = [i for i in range(number_of - 1) if given[i] < bound]
        mass, remaining = sum([portions[i] for i in candidates]), rest
        for i in candidates:
            extra = min(bound - given[i], max(1, remaining * portions[i] // mass), rest)
            given[i] = given[i] + extra
            rest = rest - extra
    return np.array([bound] + given)


def uneven(stream_key, amount, total, limit, slope):
    if amount == 2:
        one = jax.random.randint(stream_key, (), max(1, total - limit), min(limit, total - 1) + 1)
        return jnp.stack([one, total - one])
    lengths = jnp.asarray(profile(amount, total, limit, slope), jnp.int32)
    pairs = (amount - 1) // 2
    donor, taker = lengths[1:1 + 2 * pairs:2], lengths[2:2 + 2 * pairs:2]
    room = jnp.minimum(donor - 1, limit - taker)
    passed = jax.random.randint(jax.random.fold_in(stream_key, 1), (pairs,), 0, 1 << 20) % (room + 1)
    lengths = lengths.at[1:1 + 2 * pairs:2].set(donor - passed).at[2:2 + 2 * pairs:2].set(taker + passed)
    return lengths[jax.random.permutation(jax.random.fold_in(stream_key, 2), amount)]


def bell_draw(key, dims, spread, bound, cuts=(), kind=jnp.bfloat16):
    loudness = block_scale(key, dims, cuts, -0.22, 0.18) if cuts else 1.0
    values = jax.random.normal(key, dims, jnp.float32) * spread * loudness
    return jnp.minimum(jnp.maximum(values, -bound), bound).astype(kind)


def setup_inputs(seed: int = 0) -> dict:
    key_list = jax.random.split(jax.random.key(seed), 19)
    coords = draw_coords(jax.random.fold_in(key_list[18], 71), 0)
    noise = bell_draw(key_list[1], (3, WINDOWS, QW), 1.0, 6.0, ((1, 128), (2, 2)), jnp.float32)
    sigma = jnp.clip(jnp.exp(jax.random.uniform(key_list[2], (1,), jnp.float32, math.log(0.25), math.log(1.0))), 0.25, 1.0)
    atom_single = bell_draw(key_list[3], (WINDOWS, QW, C), 1.0, 6.0, ((0, 128), (1, 2)))
    token_single = bell_draw(key_list[4], (TOKENS, C_S), 1.0, 6.0, ((0, 128),))
    atom_token = jax.vmap(lambda own: jnp.searchsorted(jnp.cumsum(uneven(own, TOKW, QW, QW // 2, 2)), jnp.arange(QW), side="right"))(jax.random.split(key_list[5], WINDOWS)).reshape((WINDOWS, QW)).astype(jnp.int32)
    window_count = draw_window_count(jax.random.fold_in(key_list[18], 71), 0)
    pair_bias = draw_pair_bias(jax.random.fold_in(key_list[18], 71), 0)
    token_weight = bell_draw(key_list[8], (C_S, C), C_S ** -0.5, 0.3125)
    cond_gain = jnp.clip(1.0 + 0.15 * jax.random.normal(key_list[9], (C,), jnp.float32), 0.25, 1.75)
    position_weight = bell_draw(key_list[10], (3, C), 3 ** -0.5, 3.5, (), jnp.float32)
    ada_weight = bell_draw(key_list[11], (BLOCKS, 6, C, C), C ** -0.5, 0.5)
    ada_bias = bell_draw(key_list[12], (BLOCKS, 6, C), 1.0, 4.0, (), jnp.float32)
    attn_weight = bell_draw(key_list[13], (BLOCKS, 4, C, C), C ** -0.5, 0.5, ((3, 2),))
    out_weight = bell_draw(key_list[14], (BLOCKS, C, C), C ** -0.5, 0.5, ((1, 2),))
    gateup_weight = bell_draw(key_list[15], (BLOCKS, 2, C, HID), C ** -0.5, 0.5)
    down_weight = bell_draw(key_list[16], (BLOCKS, HID, C), HID ** -0.5, 0.375)
    final_weight = bell_draw(key_list[17], (3, C), C ** -0.5, 0.5)
    return {"coords": coords, "noise": noise, "sigma": sigma, "atom_single": atom_single, "token_single": token_single, "atom_token": atom_token, "window_count": window_count, "pair_bias": pair_bias, "token_weight": token_weight, "cond_gain": cond_gain, "position_weight": position_weight, "ada_weight": ada_weight, "ada_bias": ada_bias, "attn_weight": attn_weight, "out_weight": out_weight, "gateup_weight": gateup_weight, "down_weight": down_weight, "final_weight": final_weight}


EPSILON = 1e-05

def layer_norm(values):
    average = lax.optimization_barrier(jnp.mean(values, axis=-1, keepdims=True))
    centred = values - average
    variance = lax.optimization_barrier(jnp.mean(centred * centred, axis=-1, keepdims=True))
    return centred * lax.rsqrt(variance + EPSILON)

def lookup_tokens(tokens_here, local_token):
    token_grid = tokens_here.reshape(local_token.shape[0], TOKW, -1).astype(jnp.float32)
    one_hot = (local_token[:, :, None] == jnp.arange(TOKW, dtype=jnp.int32)).astype(jnp.float32)
    return jnp.einsum('wqt,wtc->wqc', one_hot, token_grid).astype(jnp.bfloat16)

def window_net(single, looked, scaled, pair_terms, weights_all):
    cond_gain, position_weight, ada_weight, ada_bias, attn_weight, out_weight, gateup_weight, down_weight, final_weight = weights_all
    condition = single.astype(jnp.float32) + looked.astype(jnp.float32)
    cond_norm = (layer_norm(condition) * cond_gain).astype(jnp.bfloat16)
    stream = condition + jnp.einsum('kwq,kc->wqc', scaled, position_weight, precision=lax.Precision.HIGHEST)
    window_total, row_count = (single.shape[0], single.shape[1])
    for block_index in range(BLOCKS):
        ada_terms = jnp.einsum('wqc,jcd->jwqd', cond_norm.astype(jnp.float32), ada_weight[block_index].astype(jnp.float32)) + ada_bias[block_index][:, None, None, :]
        normed = (layer_norm(stream) * jax.nn.sigmoid(ada_terms[0]) + ada_terms[1]).astype(jnp.bfloat16)
        projected = jnp.einsum('wqc,jcd->jwqd', normed.astype(jnp.float32), attn_weight[block_index].astype(jnp.float32)).astype(jnp.bfloat16)
        query_rows = projected[0].reshape(window_total, row_count, -1, HEAD_DIM).astype(jnp.float32)
        key_rows = projected[1].reshape(window_total, row_count, -1, HEAD_DIM).astype(jnp.float32)
        value_rows = projected[2].reshape(window_total, row_count, -1, HEAD_DIM).astype(jnp.float32)
        gate_logits = projected[3].reshape(window_total, row_count, -1, HEAD_DIM).astype(jnp.float32)
        scores = jnp.einsum('wqhd,wkhd->hwqk', query_rows, key_rows) * HEAD_DIM ** (-0.5) + pair_terms.astype(jnp.float32)
        row_max = lax.optimization_barrier(jnp.max(scores, axis=-1, keepdims=True))
        exponent = jnp.exp(scores - row_max)
        weights = (exponent / lax.optimization_barrier(jnp.sum(exponent, axis=-1, keepdims=True))).astype(jnp.bfloat16)
        attended = jnp.einsum('hwqk,wkhd->wqhd', weights.astype(jnp.float32), value_rows) * jax.nn.sigmoid(gate_logits)
        attended = attended.astype(jnp.bfloat16).reshape(window_total, row_count, -1)
        update = jnp.einsum('wqd,dc->wqc', attended.astype(jnp.float32), out_weight[block_index].astype(jnp.float32))
        stream = stream + jax.nn.sigmoid(ada_terms[2]) * update
        normed_two = (layer_norm(stream) * jax.nn.sigmoid(ada_terms[3]) + ada_terms[4]).astype(jnp.bfloat16)
        gate_part = jnp.einsum('wqc,ch->wqh', normed_two.astype(jnp.float32), gateup_weight[block_index, 0].astype(jnp.float32))
        up_part = jnp.einsum('wqc,ch->wqh', normed_two.astype(jnp.float32), gateup_weight[block_index, 1].astype(jnp.float32))
        hidden = (jax.nn.silu(gate_part) * up_part).astype(jnp.bfloat16)
        down_part = jnp.einsum('wqh,hc->wqc', hidden.astype(jnp.float32), down_weight[block_index].astype(jnp.float32))
        stream = stream + jax.nn.sigmoid(ada_terms[5]) * down_part
    final_norm = layer_norm(stream).astype(jnp.bfloat16)
    return jnp.einsum('wqc,kc->kwq', final_norm.astype(jnp.float32), final_weight.astype(jnp.float32))

def reference(coords, noise, sigma, atom_single, token_single, atom_token, window_count, pair_bias, token_weight, cond_gain, position_weight, ada_weight, ada_bias, attn_weight, out_weight, gateup_weight, down_weight, final_weight):
    sigma_value = sigma[0]
    noisy_pos = coords + sigma_value * noise
    slot_ids = jnp.arange(WINDOWS, dtype=jnp.int32) % WIN_DEV
    block_ids = jnp.arange(WINDOWS, dtype=jnp.int32) // WIN_DEV
    live_mask = (slot_ids < window_count[block_ids]).astype(jnp.float32)
    totals = lax.optimization_barrier(jnp.sum(noisy_pos * live_mask[None, :, None], axis=(1, 2)))
    centre = totals / (QW * jnp.sum(window_count).astype(jnp.float32))
    shifted = noisy_pos - centre[:, None, None]
    inverse = 1.0 / (1.0 + sigma_value * sigma_value)
    scaled = shifted * jnp.sqrt(inverse)
    token_proj = jnp.dot(token_single, token_weight, preferred_element_type=jnp.float32).astype(jnp.bfloat16)
    weights_all = (cond_gain, position_weight, ada_weight, ada_bias, attn_weight, out_weight, gateup_weight, down_weight, final_weight)

    def one_group(group_index):
        first_window = group_index * WIN_DEV
        single = lax.dynamic_slice_in_dim(atom_single, first_window, WIN_DEV, 0)
        tokens_here = lax.dynamic_slice_in_dim(token_proj, group_index * TOK_DEV, TOK_DEV, 0)
        local_token = lax.dynamic_slice_in_dim(atom_token, first_window, WIN_DEV, 0)
        scaled_here = lax.dynamic_slice_in_dim(scaled, first_window, WIN_DEV, 1)
        pair_terms = lax.dynamic_slice_in_dim(pair_bias, first_window, WIN_DEV, 1)
        looked = lookup_tokens(tokens_here, local_token)
        return window_net(single, looked, scaled_here, pair_terms, weights_all)
    updates = lax.map(one_group, jnp.arange(N_WIN, dtype=jnp.int32))
    update_pos = jnp.moveaxis(updates, 1, 0).reshape(3, WINDOWS, QW)
    denoised = shifted * inverse + sigma_value * jnp.sqrt(inverse) * update_pos
    return denoised * live_mask[None, :, None]
```

```python
import functools
import math

import jax
import jax.numpy as jnp
from jax import lax
from jax.experimental import pallas as pl
from jax.experimental.pallas import tpu as pltpu
from jax.sharding import Mesh
from jax.sharding import PartitionSpec as P

HEADS = 4
HEAD_DIM = 32
HALF_HEADS = 2
C = 128
QW = 128
HALF = 64
HID = 256
TOKW = 16
BLOCKS = 3
EPSILON = 1e-05
WIN = ("win_0", "win_1", "win_2")
GROUP = 4
LOG2E = math.log2(math.e)
F32 = jnp.float32
BF16 = jnp.bfloat16

NN = (((1,), (0,)), ((), ()))
NT = (((1,), (1,)), ((), ()))


def mm(a, b, dims=NN):
    return lax.dot_general(a, b, dims, preferred_element_type=F32)


def norm(x):
    mean = jnp.sum(x, axis=0, keepdims=True) * (1.0 / C)
    centred = x - mean
    var = jnp.sum(centred * centred, axis=0, keepdims=True) * (1.0 / C)
    return centred, lax.rsqrt(var + EPSILON)


def kernel(
    sizes,
    sigma,
    coords,
    noise,
    single,
    tokens,
    atok,
    wcount,
    pbias,
    tokw,
    gain,
    posw,
    adaw,
    adab,
    attnw,
    outw,
    guw,
    downw,
    finw,
    out,
    s,
):
    ny, nx, nz = sizes
    y, x, z = (lax.axis_index(name) for name in WIN)
    h = lax.axis_index("head")
    other = 1 - h
    slots = coords.shape[1]
    W = slots // 2
    NP = W // 2
    mine = pl.multiple_of(h * W, W)
    theirs = pl.multiple_of(other * W, W)

    n1, n2 = 2 * nz, ny * nx
    me1, me2 = z * 2 + h, y * nx + x

    def dev1(i):
        return {"win_2": i // 2, "head": lax.rem(i, 2)}

    def dev2(i):
        return {"win_0": i // nx, "win_1": lax.rem(i, nx)}

    barrier = pltpu.get_barrier_semaphore()
    for n, me, dev in ((n1, me1, dev1), (n2, me2, dev2)):
        for j in range(1, n):
            pl.semaphore_signal(
                barrier,
                inc=1,
                device_id=dev(lax.rem(me + j, n)),
                device_id_type=pl.DeviceIdType.MESH,
            )

    count = [0]

    def fetch(src, dst):
        copy = pltpu.make_async_copy(src, dst, s.lsem.at[count[0]])
        count[0] += 1
        copy.start()
        return copy

    small = [
        fetch(coords, s.cfull),
        fetch(noise, s.nfull),
        fetch(wcount, s.wc),
    ]
    prep = [
        fetch(gain, s.gain),
        fetch(posw, s.pw),
        fetch(adab, s.adab),
        fetch(finw, s.fin),
        fetch(tokw, s.tokw),
        fetch(tokens.at[pl.ds(pl.multiple_of(h * W * TOKW, W * TOKW), W * TOKW)], s.tok),
    ]
    c_ada = fetch(adaw, s.adaw)
    c_gu = fetch(guw, s.guw)
    c_down = fetch(downw, s.downw)
    own_rows = pl.ds(pl.multiple_of(h * HALF, HALF), HALF)
    own_in = [
        fetch(single.at[pl.ds(mine, W)], s.atoms.at[:, own_rows, :]),
        fetch(atok.at[pl.ds(mine, W)], s.tokidx.at[h]),
        fetch(coords.at[:, pl.ds(mine, W)], s.cpos.at[h]),
        fetch(noise.at[:, pl.ds(mine, W)], s.npos.at[h]),
        fetch(attnw, s.attn_l),
        fetch(outw, s.out_l),
        fetch(pbias.at[:, pl.ds(mine, W)], s.bias_l),
    ]

    sig = jnp.full((1, 128), sigma[0], F32)
    inv = 1.0 / (1.0 + sig * sig)
    root = jnp.sqrt(inv)
    lane = lax.broadcasted_iota(jnp.int32, (1, 128), 1)

    for c in small:
        c.wait()
    counts = s.wc[...].astype(F32)
    win_id = (y * nx + x) * nz + z
    win_lane = lax.broadcasted_iota(jnp.int32, counts.shape, 1)
    own_count = jnp.sum(jnp.where(win_lane == win_id, counts, 0.0), axis=1, keepdims=True)
    atoms_total = QW * jnp.sum(counts, axis=1, keepdims=True)
    slot = lax.broadcasted_iota(jnp.int32, (slots, HALF), 0).astype(F32)
    live = slot < own_count
    row = jnp.zeros((1, 128), F32)
    for k in range(3):
        noisy = jnp.where(live, s.cfull[k] + sig[:, :HALF] * s.nfull[k], 0.0)
        part = jnp.sum(jnp.sum(noisy, axis=0, keepdims=True), axis=1, keepdims=True)
        row = jnp.where(lane == k, part, row)
    s.red1[me1] = row

    pl.semaphore_wait(barrier, n1 - 1 + n2 - 1)

    def remote(src, dst, send, recv, dev):
        return pltpu.make_async_remote_copy(
            src_ref=src,
            dst_ref=dst,
            send_sem=send,
            recv_sem=recv,
            device_id=dev,
            device_id_type=pl.DeviceIdType.MESH,
        )

    def spread(buf, n, me, dev, ssem, rsem):
        sends = []
        for j in range(1, n):
            c = remote(buf.at[me], buf.at[me], ssem.at[j], rsem.at[me], dev(lax.rem(me + j, n)))
            c.start()
            sends.append(c)
        return sends

    def collect(buf, n, me, dev, ssem, rsem):
        for j in range(1, n):
            src = lax.rem(me + j, n)
            remote(buf.at[src], buf.at[src], ssem.at[j], rsem.at[src], dev(src)).wait_recv()

    sends1 = spread(s.red1, n1, me1, dev1, s.ssem1, s.rsem1)

    pair = [0]

    def give(src, dst):
        i = pair[0]
        pair[0] += 1
        c = remote(src, dst, s.psend.at[i], s.precv.at[i], {"head": other})
        c.start()
        return c

    x_atoms = give(single.at[pl.ds(theirs, W)], s.atoms.at[:, own_rows, :])
    x_tok = give(atok.at[pl.ds(theirs, W)], s.tokidx.at[h])
    x_c = give(coords.at[:, pl.ds(theirs, W)], s.cpos.at[h])
    x_n = give(noise.at[:, pl.ds(theirs, W)], s.npos.at[h])
    x_attn = give(attnw, s.attn_r)
    x_out = give(outw, s.out_r)
    x_bias = give(pbias.at[:, pl.ds(theirs, W)], s.bias_r)

    def turned(values, scale=None):
        values = values.astype(F32)
        if scale is not None:
            values = values * scale
        return values.T.astype(BF16)

    for c in prep:
        c.wait()
    s.tokwT[...] = turned(s.tokw[...])
    s.gainT[...] = jnp.broadcast_to(s.gain[...], (C, C)).T
    for k in range(3):
        s.pwT[k] = jnp.broadcast_to(s.pw[k : k + 1, :], (C, C)).T
    for b in range(BLOCKS):
        for j in range(6):
            bias = jnp.broadcast_to(s.adab[b][j : j + 1, :], (C, C)).T
            s.adabT[b * 6 + j] = bias * 0.5 if j in (0, 2, 3, 5) else bias
    c_ada.wait()
    for b in range(BLOCKS):
        for j in range(6):
            s.adaT[b, j * C : (j + 1) * C, :] = turned(
                s.adaw[b, j], 0.5 if j in (0, 2, 3, 5) else None
            )
    s.tpT[...] = mm(s.tokwT[...], s.tok[...], NT).astype(BF16)
    c_gu.wait()
    c_down.wait()
    for b in range(BLOCKS):
        s.guT[b, :HID, :] = turned(s.guw[b, 0], 0.5)
        s.guT[b, HID:, :] = turned(s.guw[b, 1])
        s.downT[b] = turned(s.downw[b], 0.5)

    for c in own_in:
        c.wait()
    for c in (x_tok, x_c, x_n, x_atoms):
        c.wait()
    s.tokcat[...] = jnp.concatenate([s.tokidx[0], s.tokidx[1]], axis=1)
    for k in range(3):
        halves = [(s.cpos[a, k] + sig[:, :HALF] * s.npos[a, k]) * root[:, :HALF] for a in (0, 1)]
        s.pos[k] = jnp.concatenate(halves, axis=1)

    eye = (
        lax.broadcasted_iota(jnp.int32, (C, C), 0) == lax.broadcasted_iota(jnp.int32, (C, C), 1)
    ).astype(BF16)

    def condition(p):
        for w in range(2):
            lanes = pl.ds(w * QW, QW)
            win = 2 * p + w
            own = s.tokcat[pl.ds(win, 1), :] + win * TOKW
            ids = lax.broadcasted_iota(jnp.int32, (W * TOKW, QW), 0)
            one_hot = jnp.where(ids == own, 1.0, 0.0).astype(BF16)
            cond = mm(eye, s.atoms[win], NT) + mm(s.tpT[...], one_hot)
            centred, rstd = norm(cond)
            s.cn[:, lanes] = (centred * rstd * s.gainT[...]).astype(BF16)
            for k in range(3):
                cond = cond + s.pos[k, pl.ds(win, 1), :] * s.pwT[k]
            s.stream[p, :, lanes] = cond
        for b in range(BLOCKS):
            terms = mm(s.adaT[b], s.cn[...])
            for j in range(6):
                for w in range(2):
                    lanes = pl.ds(w * QW, QW)
                    a = terms[j * C : (j + 1) * C, w * QW : (w + 1) * QW] + s.adabT[b * 6 + j]
                    if j in (0, 2, 3, 5):
                        a = 1.0 + jnp.tanh(a)
                    s.ada[p, b * 6 + j, :, lanes] = a

    def first(p, carry):
        condition(p)
        return carry

    half = NP // 2
    lax.fori_loop(0, half, first, 0)

    collect(s.red1, n1, me1, dev1, s.ssem1, s.rsem1)
    s.red2[me2] = jnp.sum(s.red1[...], axis=0)
    sends2 = spread(s.red2, n2, me2, dev2, s.ssem2, s.rsem2)

    lax.fori_loop(half, NP, first, 0)

    x_attn.wait()
    x_out.wait()
    for b in range(BLOCKS):
        for j in range(4):
            both = jnp.concatenate(
                [s.attn_l[b, j].astype(F32), s.attn_r[b, j].astype(F32)], axis=1
            )
            s.attnT[b, j * C : (j + 1) * C, :] = turned(both, 0.5 if j == 3 else None)
        both = jnp.concatenate([s.out_l[b].astype(F32), s.out_r[b].astype(F32)], axis=0)
        s.outT[b] = turned(both, 0.25)
    x_bias.wait()

    def turn_bias(w, carry):
        for a in range(HALF_HEADS):
            for side, buf in enumerate((s.bias_l, s.bias_r)):
                i = side * HALF_HEADS + a
                s.biasT[w, :, i * QW : (i + 1) * QW] = (buf[a, w].astype(F32) * LOG2E).T
        return carry

    lax.fori_loop(0, W, turn_bias, 0)

    collect(s.red2, n2, me2, dev2, s.ssem2, s.rsem2)
    total = jnp.sum(s.red2[...], axis=0) / atoms_total
    centre = [
        jnp.sum(jnp.where(lane == k, total, 0.0), axis=1, keepdims=True) for k in range(3)
    ]
    shift = jnp.zeros((C, C), F32)
    for k in range(3):
        shift = shift + (centre[k] * root) * s.pwT[k]
    s.shift[...] = shift

    q_scale = LOG2E * HEAD_DIM ** (-0.5)
    pairs = GROUP // 2

    def begin(p, carry):
        for w in range(2):
            lanes = pl.ds(w * QW, QW)
            s.stream[p, :, lanes] = s.stream[p, :, lanes] - s.shift[...]
        return carry

    lax.fori_loop(0, NP, begin, 0)

    def block(step, carry):
        b = lax.rem(step, BLOCKS)
        base = (step // BLOCKS) * pairs

        def term(i, j, w):
            return s.ada[base + i, b * 6 + j, :, pl.ds(w * QW, QW)]

        for i in range(pairs):
            for w in range(2):
                lanes = pl.ds(w * QW, QW)
                centred, rstd = norm(s.stream[base + i, :, lanes])
                n = centred * (0.5 * rstd) * term(i, 0, w) + term(i, 1, w)
                s.n[i, :, lanes] = n.astype(BF16)
        for i in range(pairs):
            proj = mm(s.attnT[b], s.n[i])
            s.q[i] = (proj[:C] * q_scale).astype(BF16)
            s.v[i] = proj[2 * C : 3 * C].astype(BF16)
            s.gate[i] = 1.0 + jnp.tanh(proj[3 * C :])
            for w in range(2):
                s.k[2 * i + w] = proj[C : 2 * C, w * QW : (w + 1) * QW].T.astype(BF16)
        for i in range(pairs):
            for w in range(2):
                lanes = pl.ds(w * QW, QW)
                keys = s.k[2 * i + w]
                attended = []
                for hp in range(2):
                    cols = []
                    for a in range(2):
                        at = (2 * hp + a) * HEAD_DIM
                        part = [s.q[i, at : at + HEAD_DIM, lanes]]
                        if at > 0:
                            part = [jnp.zeros((at, QW), BF16)] + part
                        if at + HEAD_DIM < C:
                            part = part + [jnp.zeros((C - HEAD_DIM - at, QW), BF16)]
                        cols.append(jnp.concatenate(part, axis=0))
                    scores = mm(keys, jnp.concatenate(cols, axis=1))
                    for a in range(2):
                        hd = 2 * hp + a
                        sc = (
                            scores[:, a * QW : (a + 1) * QW]
                            + s.biasT[2 * (base + i) + w, :, hd * QW : (hd + 1) * QW]
                        )
                        e = jnp.exp2(sc - jnp.max(sc, axis=0, keepdims=True))
                        recip = 1.0 / jnp.sum(e, axis=0, keepdims=True)
                        at = hd * HEAD_DIM
                        o = mm(s.v[i, at : at + HEAD_DIM, lanes], e.astype(BF16))
                        attended.append(o * recip)
                both = jnp.concatenate(attended, axis=0) * s.gate[i, :, lanes]
                s.att[i, :, lanes] = both.astype(BF16)
        for i in range(pairs):
            update = mm(s.outT[b], s.att[i])
            for w in range(2):
                lanes = pl.ds(w * QW, QW)
                xs = s.stream[base + i, :, lanes] + term(i, 2, w) * update[:, w * QW : (w + 1) * QW]
                s.stream[base + i, :, lanes] = xs
                centred, rstd = norm(xs)
                n = centred * (0.5 * rstd) * term(i, 3, w) + term(i, 4, w)
                s.n[i, :, lanes] = n.astype(BF16)
        for i in range(pairs):
            both = mm(s.guT[b], s.n[i])
            g = both[:HID]
            s.hidden[i] = (g * (1.0 + jnp.tanh(g)) * both[HID:]).astype(BF16)
        for i in range(pairs):
            down = mm(s.downT[b], s.hidden[i])
            for w in range(2):
                lanes = pl.ds(w * QW, QW)
                s.stream[base + i, :, lanes] = (
                    s.stream[base + i, :, lanes] + term(i, 5, w) * down[:, w * QW : (w + 1) * QW]
                )
        return carry

    lax.fori_loop(0, BLOCKS * (NP // pairs), block, 0)

    final = jnp.concatenate([s.fin[...].astype(F32), jnp.zeros((5, C), F32)], axis=0).astype(BF16)

    def finish(p, carry):
        for w in range(2):
            centred, rstd = norm(s.stream[p, :, pl.ds(w * QW, QW)])
            upd = mm(final, (centred * rstd).astype(BF16))
            for k in range(3):
                s.upd[k, pl.ds(2 * p + w, 1), :] = upd[k : k + 1, :]
        return carry

    lax.fori_loop(0, NP, finish, 0)
    x_upd = give(s.upd, s.updr)

    def write(source, first_slot):
        first_slot = pl.multiple_of(first_slot, W)
        ids = (lax.broadcasted_iota(jnp.int32, (W, HALF), 0) + first_slot).astype(F32)
        alive = ids < own_count
        for k in range(3):
            both = source[k]
            upd = jnp.where(h == 0, both[:, :HALF], both[:, HALF:])
            here = pl.ds(first_slot, W)
            noisy = s.cfull[k, here, :] + sig[:, :HALF] * s.nfull[k, here, :]
            shifted = noisy - centre[k]
            value = shifted * inv[:, :HALF] + (sig * root)[:, :HALF] * upd
            out[k, here, :] = jnp.where(alive, value, 0.0)

    write(s.upd, mine)
    x_upd.wait()
    write(s.updr, theirs)
    for c in sends1 + sends2:
        c.wait_send()


class Scratch:
    pass


def scratch_of(slots, nz, nxy):
    win_total = nz * nxy
    W = slots // 2
    NP = W // 2
    G = GROUP // 2
    V = pltpu.VMEM
    return {
        "cfull": V((3, slots, HALF), F32),
        "nfull": V((3, slots, HALF), F32),
        "wc": V((1, win_total), jnp.int32),
        "gain": V((1, C), F32),
        "pw": V((3, C), F32),
        "adab": V((BLOCKS, 6, C), F32),
        "fin": V((3, C), BF16),
        "tokw": V((3 * C, C), BF16),
        "tok": V((W * TOKW, 3 * C), BF16),
        "adaw": V((BLOCKS, 6, C, C), BF16),
        "guw": V((BLOCKS, 2, C, HID), BF16),
        "downw": V((BLOCKS, HID, C), BF16),
        "atoms": V((W, QW, C), BF16),
        "tokidx": V((2, W, HALF), jnp.int32),
        "cpos": V((2, 3, W, HALF), F32),
        "npos": V((2, 3, W, HALF), F32),
        "attn_l": V((BLOCKS, 4, C, HALF), BF16),
        "attn_r": V((BLOCKS, 4, C, HALF), BF16),
        "out_l": V((BLOCKS, HALF, C), BF16),
        "out_r": V((BLOCKS, HALF, C), BF16),
        "bias_l": V((2, W, QW, QW), BF16),
        "bias_r": V((2, W, QW, QW), BF16),
        "red1": V((2 * nz, 1, 128), F32),
        "red2": V((nxy, 1, 128), F32),
        "tokwT": V((C, 3 * C), BF16),
        "gainT": V((C, C), F32),
        "pwT": V((3, C, C), F32),
        "adabT": V((BLOCKS * 6, C, C), F32),
        "adaT": V((BLOCKS, 6 * C, C), BF16),
        "attnT": V((BLOCKS, 4 * C, C), BF16),
        "outT": V((BLOCKS, C, C), BF16),
        "guT": V((BLOCKS, 2 * HID, C), BF16),
        "downT": V((BLOCKS, C, HID), BF16),
        "tpT": V((C, W * TOKW), BF16),
        "tokcat": V((W, QW), jnp.int32),
        "pos": V((3, W, QW), F32),
        "cn": V((C, 2 * QW), BF16),
        "stream": V((NP, C, 2 * QW), F32),
        "ada": V((NP, BLOCKS * 6, C, 2 * QW), F32),
        "biasT": V((W, QW, HEADS * QW), F32),
        "shift": V((C, C), F32),
        "n": V((G, C, 2 * QW), BF16),
        "q": V((G, C, 2 * QW), BF16),
        "k": V((2 * G, QW, C), BF16),
        "v": V((G, C, 2 * QW), BF16),
        "gate": V((G, C, 2 * QW), F32),
        "att": V((G, C, 2 * QW), BF16),
        "hidden": V((G, HID, 2 * QW), BF16),
        "upd": V((3, W, QW), F32),
        "updr": V((3, W, QW), F32),
        "lsem": pltpu.SemaphoreType.DMA((20,)),
        "ssem1": pltpu.SemaphoreType.DMA((2 * nz,)),
        "rsem1": pltpu.SemaphoreType.DMA((2 * nz,)),
        "ssem2": pltpu.SemaphoreType.DMA((nxy,)),
        "rsem2": pltpu.SemaphoreType.DMA((nxy,)),
        "psend": pltpu.SemaphoreType.DMA((8,)),
        "precv": pltpu.SemaphoreType.DMA((8,)),
    }


def make_local(sizes):
    def local(
        coords,
        noise,
        sigma,
        atom_single,
        token_single,
        atom_token,
        window_count,
        pair_bias,
        token_weight,
        cond_gain,
        position_weight,
        ada_weight,
        ada_bias,
        attn_weight,
        out_weight,
        gateup_weight,
        down_weight,
        final_weight,
    ):
        slots = coords.shape[1]
        ny, nx, nz = sizes
        scratch = scratch_of(slots, nz, ny * nx)
        names = list(scratch)

        def body(*refs):
            s = Scratch()
            for name, ref in zip(names, refs[19:]):
                setattr(s, name, ref)
            kernel(sizes, *refs[:19], s)

        any_spec = pl.BlockSpec(memory_space=pl.ANY)
        return pl.pallas_call(
            body,
            out_shape=jax.ShapeDtypeStruct(coords.shape, F32),
            in_specs=[pl.BlockSpec(memory_space=pltpu.SMEM)] + [any_spec] * 17,
            out_specs=pl.BlockSpec(memory_space=pltpu.VMEM),
            scratch_shapes=[scratch[name] for name in names],
            compiler_params=pltpu.CompilerParams(
                collective_id=0, has_side_effects=True, vmem_limit_bytes=60 * 1024 * 1024
            ),
            name="denoise",
        )(
            sigma,
            coords,
            noise,
            atom_single,
            token_single,
            atom_token,
            window_count.reshape(1, -1),
            pair_bias,
            token_weight,
            cond_gain.reshape(1, -1),
            position_weight,
            ada_weight,
            ada_bias,
            attn_weight,
            out_weight,
            gateup_weight,
            down_weight,
            final_weight,
        )

    return local


def solution(mesh):
    devices = mesh.devices
    head = mesh.shape["head"]
    sizes = (4, 4, 8) if devices.size == 256 else (2, 2, devices.size // (4 * head))
    torus = Mesh(devices.reshape(*sizes, head), WIN + ("head",))
    in_specs = (
        P(None, WIN, "head"),
        P(None, WIN, "head"),
        P(),
        P(WIN, "head", None),
        P(WIN, None),
        P(WIN, "head"),
        P(),
        P("head", WIN, None, None),
        P(),
        P(),
        P(),
        P(),
        P(),
        P(None, None, None, "head"),
        P(None, "head", None),
        P(),
        P(),
        P(),
    )
    out_specs = P(None, WIN, "head")
    return jax.shard_map(
        make_local(sizes), mesh=torus, in_specs=in_specs, out_specs=out_specs, check_vma=False
    )
```

```python
import functools
import math

import jax
import jax.numpy as jnp
from jax import lax
from jax.experimental import pallas as pl
from jax.experimental.pallas import tpu as pltpu
from jax.sharding import Mesh
from jax.sharding import PartitionSpec as P

HEADS = 4
HEAD_DIM = 32
HALF_HEADS = 2
C = 128
QW = 128
HALF = 64
HID = 256
TOKW = 16
BLOCKS = 3
EPSILON = 1e-05
WIN = ("win_0", "win_1", "win_2")
LOG2E = math.log2(math.e)
F32 = jnp.float32
BF16 = jnp.bfloat16

NN = (((1,), (0,)), ((), ()))
NT = (((1,), (1,)), ((), ()))


def mm(a, b, dims=NN):
    return lax.dot_general(a, b, dims, preferred_element_type=F32)


def norm(x):
    mean = jnp.sum(x, axis=0, keepdims=True) * (1.0 / C)
    centred = x - mean
    var = jnp.sum(centred * centred, axis=0, keepdims=True) * (1.0 / C)
    return centred, lax.rsqrt(var + EPSILON)


def kernel(
    sizes,
    sigma,
    coords,
    noise,
    single,
    tokens,
    atok,
    wcount,
    pbias,
    tokw,
    gain,
    posw,
    adaw,
    adab,
    attnw,
    outw,
    guw,
    downw,
    finw,
    out,
    s,
):
    ny, nx, nz = sizes
    y, x, z = (lax.axis_index(name) for name in WIN)
    h = lax.axis_index("head")
    other = 1 - h
    slots = coords.shape[1]
    W = slots // 2
    NP = W // 2
    mine = pl.multiple_of(h * W, W)
    theirs = pl.multiple_of(other * W, W)

    n1, n2 = 2 * nz, ny * nx
    me1, me2 = z * 2 + h, y * nx + x

    def dev1(i):
        return {"win_2": i // 2, "head": lax.rem(i, 2)}

    def dev2(i):
        return {"win_0": i // nx, "win_1": lax.rem(i, nx)}

    barrier = pltpu.get_barrier_semaphore()
    for n, me, dev in ((n1, me1, dev1), (n2, me2, dev2)):
        for j in range(1, n):
            pl.semaphore_signal(
                barrier,
                inc=1,
                device_id=dev(lax.rem(me + j, n)),
                device_id_type=pl.DeviceIdType.MESH,
            )

    count = [0]

    def fetch(src, dst):
        copy = pltpu.make_async_copy(src, dst, s.lsem.at[count[0]])
        count[0] += 1
        copy.start()
        return copy

    small = [
        fetch(coords, s.cfull),
        fetch(noise, s.nfull),
        fetch(wcount, s.wc),
        fetch(sigma, s.sig),
    ]
    prep = [
        fetch(gain, s.gain),
        fetch(posw, s.pw),
        fetch(adab, s.adab),
        fetch(finw, s.fin),
        fetch(tokw, s.tokw),
        fetch(tokens.at[pl.ds(pl.multiple_of(h * W * TOKW, W * TOKW), W * TOKW)], s.tok),
    ]
    c_ada = fetch(adaw, s.adaw)
    c_gu = fetch(guw, s.guw)
    c_down = fetch(downw, s.downw)
    own_rows = pl.ds(pl.multiple_of(h * HALF, HALF), HALF)
    own_in = [
        fetch(single.at[pl.ds(mine, W)], s.atoms.at[:, own_rows, :]),
        fetch(atok.at[pl.ds(mine, W)], s.tokidx.at[h]),
        fetch(coords.at[:, pl.ds(mine, W)], s.cpos.at[h]),
        fetch(noise.at[:, pl.ds(mine, W)], s.npos.at[h]),
        fetch(attnw, s.attnT.at[:, :, pl.ds(0, HALF), :]),
        fetch(outw, s.out_l),
        fetch(pbias.at[:, pl.ds(mine, W)], s.bias_l),
    ]

    lane = lax.broadcasted_iota(jnp.int32, (1, 128), 1)

    for c in small:
        c.wait()
    sig = jnp.broadcast_to(s.sig[...], (1, 128))
    inv = 1.0 / (1.0 + sig * sig)
    root = jnp.sqrt(inv)
    counts = s.wc[...].astype(F32)
    win_id = (y * nx + x) * nz + z
    win_lane = lax.broadcasted_iota(jnp.int32, counts.shape, 1)
    own_count = jnp.sum(jnp.where(win_lane == win_id, counts, 0.0), axis=1, keepdims=True)
    atoms_total = QW * jnp.sum(counts, axis=1, keepdims=True)
    slot = lax.broadcasted_iota(jnp.int32, (slots, HALF), 0).astype(F32)
    live = slot < own_count
    row = jnp.zeros((1, 128), F32)
    for k in range(3):
        noisy = jnp.where(live, s.cfull[k] + sig[:, :HALF] * s.nfull[k], 0.0)
        part = jnp.sum(jnp.sum(noisy, axis=0, keepdims=True), axis=1, keepdims=True)
        row = jnp.where(lane == k, part, row)
    s.red1[me1] = row

    pl.semaphore_wait(barrier, n1 - 1 + n2 - 1)

    def remote(src, dst, send, recv, dev):
        return pltpu.make_async_remote_copy(
            src_ref=src,
            dst_ref=dst,
            send_sem=send,
            recv_sem=recv,
            device_id=dev,
            device_id_type=pl.DeviceIdType.MESH,
        )

    def spread(buf, n, me, dev, ssem, rsem):
        sends = []
        for j in range(1, n):
            c = remote(buf.at[me], buf.at[me], ssem.at[j], rsem.at[me], dev(lax.rem(me + j, n)))
            c.start()
            sends.append(c)
        return sends

    def collect(buf, n, me, dev, ssem, rsem):
        for j in range(1, n):
            src = lax.rem(me + j, n)
            remote(buf.at[src], buf.at[src], ssem.at[j], rsem.at[src], dev(src)).wait_recv()

    sends1 = spread(s.red1, n1, me1, dev1, s.ssem1, s.rsem1)

    pair = [0]

    def give(src, dst):
        i = pair[0]
        pair[0] += 1
        c = remote(src, dst, s.psend.at[i], s.precv.at[i], {"head": other})
        c.start()
        return c

    x_atoms = give(single.at[pl.ds(theirs, W)], s.atoms.at[:, own_rows, :])
    x_tok = give(atok.at[pl.ds(theirs, W)], s.tokidx.at[h])
    x_c = give(coords.at[:, pl.ds(theirs, W)], s.cpos.at[h])
    x_n = give(noise.at[:, pl.ds(theirs, W)], s.npos.at[h])
    x_attn = give(attnw, s.attnT.at[:, :, pl.ds(HALF, HALF), :])
    x_out = give(outw, s.out_r)
    x_bias = give(pbias.at[:, pl.ds(theirs, W)], s.bias_r)

    def turned(values, scale=None):
        values = values.astype(F32)
        if scale is not None:
            values = values * scale
        return values.T.astype(BF16)

    for c in prep:
        c.wait()
    s.tokwT[...] = turned(s.tokw[...])
    s.gainT[...] = jnp.broadcast_to(s.gain[...], (C, C)).T
    for k in range(3):
        s.pwT[k] = jnp.broadcast_to(s.pw[k : k + 1, :], (C, C)).T
    for b in range(BLOCKS):
        for j in range(6):
            bias = jnp.broadcast_to(s.adab[b][j : j + 1, :], (C, C)).T
            s.adabT[b * 6 + j] = bias * 0.5 if j in (0, 2, 3, 5) else bias
    c_ada.wait()
    for b in range(BLOCKS):
        for j in range(6):
            s.adaT[b, j * C : (j + 1) * C, :] = turned(
                s.adaw[b, j], 0.5 if j in (0, 2, 3, 5) else None
            )
    s.tpT[...] = mm(s.tokwT[...], s.tok[...], NT).astype(BF16)
    c_gu.wait()
    c_down.wait()
    for b in range(BLOCKS):
        s.guT[b, :HID, :] = turned(s.guw[b, 0], 0.5)
        s.guT[b, HID:, :] = turned(s.guw[b, 1])
        s.downT[b] = turned(s.downw[b], 0.5)

    for c in own_in:
        c.wait()
    for c in (x_tok, x_c, x_n, x_atoms):
        c.wait()
    s.tokcat[...] = jnp.concatenate([s.tokidx[0], s.tokidx[1]], axis=1)
    for k in range(3):
        halves = [(s.cpos[a, k] + sig[:, :HALF] * s.npos[a, k]) * root[:, :HALF] for a in (0, 1)]
        s.pos[k] = jnp.concatenate(halves, axis=1)

    eye = (
        lax.broadcasted_iota(jnp.int32, (C, C), 0) == lax.broadcasted_iota(jnp.int32, (C, C), 1)
    ).astype(BF16)

    def condition(p):
        for w in range(2):
            lanes = pl.ds(w * QW, QW)
            win = 2 * p + w
            own = s.tokcat[pl.ds(win, 1), :] + win * TOKW
            ids = lax.broadcasted_iota(jnp.int32, (W * TOKW, QW), 0)
            one_hot = jnp.where(ids == own, 1.0, 0.0).astype(BF16)
            cond = mm(eye, s.atoms[win], NT) + mm(s.tpT[...], one_hot)
            centred, rstd = norm(cond)
            s.cn[:, lanes] = (centred * rstd * s.gainT[...]).astype(BF16)
            for k in range(3):
                cond = cond + s.pos[k, pl.ds(win, 1), :] * s.pwT[k]
            s.stream[p, :, lanes] = cond
        for b in range(BLOCKS):
            terms = mm(s.adaT[b], s.cn[...])
            for j in range(6):
                for w in range(2):
                    lanes = pl.ds(w * QW, QW)
                    a = terms[j * C : (j + 1) * C, w * QW : (w + 1) * QW] + s.adabT[b * 6 + j]
                    if j in (0, 2, 3, 5):
                        a = 1.0 + jnp.tanh(a)
                    s.ada[p, b * 6 + j, :, lanes] = a

    def first(p, carry):
        condition(p)
        return carry

    half = NP // 2
    lax.fori_loop(0, half, first, 0)

    collect(s.red1, n1, me1, dev1, s.ssem1, s.rsem1)
    s.red2[me2] = jnp.sum(s.red1[...], axis=0)
    sends2 = spread(s.red2, n2, me2, dev2, s.ssem2, s.rsem2)

    lax.fori_loop(half, NP, first, 0)

    x_attn.wait()
    x_out.wait()
    for b in range(BLOCKS):
        s.attnT[b, 3] = (s.attnT[b, 3].astype(F32) * 0.5).astype(BF16)
        both = jnp.concatenate([s.out_l[b].astype(F32), s.out_r[b].astype(F32)], axis=0)
        s.outT[b] = turned(both, 0.25)
    x_bias.wait()

    def turn_bias(w, carry):
        for a in range(HALF_HEADS):
            for side, buf in enumerate((s.bias_l, s.bias_r)):
                i = side * HALF_HEADS + a
                s.biasT[w, :, i * QW : (i + 1) * QW] = (buf[a, w].astype(F32) * LOG2E).T
        return carry

    lax.fori_loop(0, W, turn_bias, 0)

    collect(s.red2, n2, me2, dev2, s.ssem2, s.rsem2)
    total = jnp.sum(s.red2[...], axis=0) / atoms_total
    centre = [
        jnp.sum(jnp.where(lane == k, total, 0.0), axis=1, keepdims=True) for k in range(3)
    ]
    shift = jnp.zeros((C, C), F32)
    for k in range(3):
        shift = shift + (centre[k] * root) * s.pwT[k]
    s.shift[...] = shift

    q_scale = LOG2E * HEAD_DIM ** (-0.5)
    quads = NP // 2

    def begin(p, carry):
        for w in range(2):
            lanes = pl.ds(w * QW, QW)
            s.stream[p, :, lanes] = s.stream[p, :, lanes] - s.shift[...]
        return carry

    lax.fori_loop(0, NP, begin, 0)

    def halves(w):
        return slice(w * QW, (w + 1) * QW)

    def project(b, quad, par):
        def normed(i, w):
            p, lanes = 2 * quad + i, halves(w)
            centred, rstd = norm(s.stream[p, :, lanes])
            n = centred * (0.5 * rstd) * s.ada[p, b * 6, :, lanes] + s.ada[p, b * 6 + 1, :, lanes]
            s.n[i, :, lanes] = n.astype(BF16)

        def proj(i):
            y = mm(s.attnT[b].reshape(4 * C, C), s.n[i])
            s.q[par, i] = (y[:C] * q_scale).astype(BF16)
            for w in range(2):
                s.k[par, 2 * i + w] = y[C : 2 * C, halves(w)].T.astype(BF16)
            s.v[par, i] = y[2 * C : 3 * C].astype(BF16)
            s.gate[par, i] = 1.0 + jnp.tanh(y[3 * C :])

        return [
            functools.partial(normed, 0, 0),
            functools.partial(normed, 0, 1),
            functools.partial(proj, 0),
            functools.partial(normed, 1, 0),
            functools.partial(normed, 1, 1),
            functools.partial(proj, 1),
        ]

    def attend(b, quad, par):
        held = {}

        def scores(i, w, hp):
            cols = []
            for a in range(2):
                at = (2 * hp + a) * HEAD_DIM
                part = [s.q[par, i, at : at + HEAD_DIM, halves(w)]]
                if at > 0:
                    part = [jnp.zeros((at, QW), BF16)] + part
                if at + HEAD_DIM < C:
                    part = part + [jnp.zeros((C - HEAD_DIM - at, QW), BF16)]
                cols.append(jnp.concatenate(part, axis=0))
            held[i, w, hp] = mm(s.k[par, 2 * i + w], jnp.concatenate(cols, axis=1))

        def mix(i, w, hp):
            both = held.pop((i, w, hp))
            for a in range(2):
                hd = 2 * hp + a
                at = slice(hd * HEAD_DIM, (hd + 1) * HEAD_DIM)
                sc = both[:, halves(a)] + s.biasT[4 * quad + 2 * i + w, :, halves(hd)]
                e = jnp.exp2(sc - jnp.max(sc, axis=0, keepdims=True))
                recip = 1.0 / jnp.sum(e, axis=0, keepdims=True)
                o = mm(s.v[par, i, at, halves(w)], e.astype(BF16))
                s.att[par, i, at, halves(w)] = (
                    o * recip * s.gate[par, i, at, halves(w)]
                ).astype(BF16)

        units = [(i, w, hp) for i in range(2) for w in range(2) for hp in range(2)]
        out = [functools.partial(scores, *units[0])]
        for n, unit in enumerate(units):
            if n + 1 < len(units):
                out.append(functools.partial(scores, *units[n + 1]))
            out.append(functools.partial(mix, *unit))
        return out

    def add_attended(b, quad, par):
        def piece(i):
            p = 2 * quad + i
            update = mm(s.outT[b], s.att[par, i])
            for w in range(2):
                lanes = halves(w)
                xs = s.stream[p, :, lanes] + s.ada[p, b * 6 + 2, :, lanes] * update[:, lanes]
                s.mid[par, i, :, lanes] = xs
                centred, rstd = norm(xs)
                n = centred * (0.5 * rstd) * s.ada[p, b * 6 + 3, :, lanes]
                s.n2[par, i, :, lanes] = (n + s.ada[p, b * 6 + 4, :, lanes]).astype(BF16)

        return [functools.partial(piece, i) for i in range(2)]

    def transition(b, quad, par):
        def up(i):
            both = mm(s.guT[b], s.n2[par, i])
            g = both[:HID]
            s.hidden[i] = (g * (1.0 + jnp.tanh(g)) * both[HID:]).astype(BF16)

        def down(i):
            p = 2 * quad + i
            d = mm(s.downT[b], s.hidden[i])
            for w in range(2):
                lanes = halves(w)
                s.stream[p, :, lanes] = (
                    s.mid[par, i, :, lanes] + s.ada[p, b * 6 + 5, :, lanes] * d[:, lanes]
                )

        return [
            functools.partial(up, 0),
            functools.partial(up, 1),
            functools.partial(down, 0),
            functools.partial(down, 1),
        ]

    steps = (project, attend, add_attended, transition)

    def slot_of(b, t, first_step, last_step):
        work = []
        for n in range(first_step, last_step + 1):
            quad = (t - n) % quads
            block_of = b - (n - t + quads - 1) // quads if n > t else b
            parity = (t - n) % 2
            pieces = steps[n](block_of, quad, parity if n == 0 else parity)
            work.append((n, pieces))
        order = []
        for n, pieces in work:
            for at, piece in enumerate(pieces):
                order.append(((at + 0.5) / len(pieces), -n, piece))
        for _, _, piece in sorted(order, key=lambda entry: entry[:2]):
            piece()

    for t in range(quads):
        slot_of(0, t, 0, min(t, 3))

    def middle(b, carry):
        for t in range(quads):
            slot_of(b, t, 0, 3)
        return carry

    lax.fori_loop(1, BLOCKS, middle, 0)
    for t in range(3):
        slot_of(BLOCKS, t, t + 1, 3)

    final = jnp.concatenate([s.fin[...].astype(F32), jnp.zeros((5, C), F32)], axis=0).astype(BF16)

    def finish(p, carry):
        for w in range(2):
            centred, rstd = norm(s.stream[p, :, pl.ds(w * QW, QW)])
            upd = mm(final, (centred * rstd).astype(BF16))
            for k in range(3):
                s.upd[k, pl.ds(2 * p + w, 1), :] = upd[k : k + 1, :]
        return carry

    lax.fori_loop(0, NP, finish, 0)
    x_upd = give(s.upd, s.updr)

    def write(source, first_slot):
        first_slot = pl.multiple_of(first_slot, W)
        ids = (lax.broadcasted_iota(jnp.int32, (W, HALF), 0) + first_slot).astype(F32)
        alive = ids < own_count
        for k in range(3):
            both = source[k]
            upd = jnp.where(h == 0, both[:, :HALF], both[:, HALF:])
            here = pl.ds(first_slot, W)
            noisy = s.cfull[k, here, :] + sig[:, :HALF] * s.nfull[k, here, :]
            shifted = noisy - centre[k]
            value = shifted * inv[:, :HALF] + (sig * root)[:, :HALF] * upd
            out[k, here, :] = jnp.where(alive, value, 0.0)

    write(s.upd, mine)
    x_upd.wait()
    write(s.updr, theirs)
    for c in sends1 + sends2:
        c.wait_send()


class Scratch:
    pass


def scratch_of(slots, nz, nxy):
    win_total = nz * nxy
    W = slots // 2
    NP = W // 2
    V = pltpu.VMEM
    return {
        "cfull": V((3, slots, HALF), F32),
        "nfull": V((3, slots, HALF), F32),
        "wc": V((1, win_total), jnp.int32),
        "sig": V((1, 1), F32),
        "gain": V((1, C), F32),
        "pw": V((3, C), F32),
        "adab": V((BLOCKS, 6, C), F32),
        "fin": V((3, C), BF16),
        "tokw": V((3 * C, C), BF16),
        "tok": V((W * TOKW, 3 * C), BF16),
        "adaw": V((BLOCKS, 6, C, C), BF16),
        "guw": V((BLOCKS, 2, C, HID), BF16),
        "downw": V((BLOCKS, HID, C), BF16),
        "atoms": V((W, QW, C), BF16),
        "tokidx": V((2, W, HALF), jnp.int32),
        "cpos": V((2, 3, W, HALF), F32),
        "npos": V((2, 3, W, HALF), F32),
        "out_l": V((BLOCKS, HALF, C), BF16),
        "out_r": V((BLOCKS, HALF, C), BF16),
        "bias_l": V((2, W, QW, QW), BF16),
        "bias_r": V((2, W, QW, QW), BF16),
        "red1": V((2 * nz, 1, 128), F32),
        "red2": V((nxy, 1, 128), F32),
        "tokwT": V((C, 3 * C), BF16),
        "gainT": V((C, C), F32),
        "pwT": V((3, C, C), F32),
        "adabT": V((BLOCKS * 6, C, C), F32),
        "adaT": V((BLOCKS, 6 * C, C), BF16),
        "attnT": V((BLOCKS, 4, C, C), BF16),
        "outT": V((BLOCKS, C, C), BF16),
        "guT": V((BLOCKS, 2 * HID, C), BF16),
        "downT": V((BLOCKS, C, HID), BF16),
        "tpT": V((C, W * TOKW), BF16),
        "tokcat": V((W, QW), jnp.int32),
        "pos": V((3, W, QW), F32),
        "cn": V((C, 2 * QW), BF16),
        "stream": V((NP, C, 2 * QW), F32),
        "ada": V((NP, BLOCKS * 6, C, 2 * QW), F32),
        "biasT": V((W, QW, HEADS * QW), F32),
        "shift": V((C, C), F32),
        "n": V((2, C, 2 * QW), BF16),
        "q": V((2, 2, C, 2 * QW), BF16),
        "k": V((2, 4, QW, C), BF16),
        "v": V((2, 2, C, 2 * QW), BF16),
        "gate": V((2, 2, C, 2 * QW), F32),
        "att": V((2, 2, C, 2 * QW), BF16),
        "mid": V((2, 2, C, 2 * QW), F32),
        "n2": V((2, 2, C, 2 * QW), BF16),
        "hidden": V((2, HID, 2 * QW), BF16),
        "upd": V((3, W, QW), F32),
        "updr": V((3, W, QW), F32),
        "lsem": pltpu.SemaphoreType.DMA((20,)),
        "ssem1": pltpu.SemaphoreType.DMA((2 * nz,)),
        "rsem1": pltpu.SemaphoreType.DMA((2 * nz,)),
        "ssem2": pltpu.SemaphoreType.DMA((nxy,)),
        "rsem2": pltpu.SemaphoreType.DMA((nxy,)),
        "psend": pltpu.SemaphoreType.DMA((8,)),
        "precv": pltpu.SemaphoreType.DMA((8,)),
    }


def make_local(sizes):
    def local(
        coords,
        noise,
        sigma,
        atom_single,
        token_single,
        atom_token,
        window_count,
        pair_bias,
        token_weight,
        cond_gain,
        position_weight,
        ada_weight,
        ada_bias,
        attn_weight,
        out_weight,
        gateup_weight,
        down_weight,
        final_weight,
    ):
        slots = coords.shape[1]
        ny, nx, nz = sizes
        scratch = scratch_of(slots, nz, ny * nx)
        names = list(scratch)

        def body(*refs):
            s = Scratch()
            for name, ref in zip(names, refs[19:]):
                setattr(s, name, ref)
            kernel(sizes, *refs[:19], s)

        any_spec = pl.BlockSpec(memory_space=pl.ANY)
        return pl.pallas_call(
            body,
            out_shape=jax.ShapeDtypeStruct(coords.shape, F32),
            in_specs=[any_spec] * 18,
            out_specs=pl.BlockSpec(memory_space=pltpu.VMEM),
            scratch_shapes=[scratch[name] for name in names],
            compiler_params=pltpu.CompilerParams(
                collective_id=0, has_side_effects=True, vmem_limit_bytes=60 * 1024 * 1024
            ),
            name="denoise",
        )(
            sigma.reshape(1, 1),
            coords,
            noise,
            atom_single,
            token_single,
            atom_token,
            window_count.reshape(1, -1),
            pair_bias,
            token_weight,
            cond_gain.reshape(1, -1),
            position_weight,
            ada_weight,
            ada_bias,
            jnp.swapaxes(attn_weight, 2, 3),
            out_weight,
            gateup_weight,
            down_weight,
            final_weight,
        )

    return local


def solution(mesh):
    devices = mesh.devices
    head = mesh.shape["head"]
    sizes = (4, 4, 8) if devices.size == 256 else (2, 2, devices.size // (4 * head))
    torus = Mesh(devices.reshape(*sizes, head), WIN + ("head",))
    in_specs = (
        P(None, WIN, "head"),
        P(None, WIN, "head"),
        P(),
        P(WIN, "head", None),
        P(WIN, None),
        P(WIN, "head"),
        P(),
        P("head", WIN, None, None),
        P(),
        P(),
        P(),
        P(),
        P(),
        P(None, None, None, "head"),
        P(None, "head", None),
        P(),
        P(),
        P(),
    )
    out_specs = P(None, WIN, "head")
    return jax.shard_map(
        make_local(sizes), mesh=torus, in_specs=in_specs, out_specs=out_specs, check_vma=False
    )
```

```python
import functools
import math

import jax
import jax.numpy as jnp
from jax import lax
from jax.experimental import pallas as pl
from jax.experimental.pallas import tpu as pltpu
from jax.sharding import Mesh
from jax.sharding import PartitionSpec as P

HEADS = 4
HEAD_DIM = 32
HALF_HEADS = 2
C = 128
QW = 128
HALF = 64
HID = 256
TOKW = 16
BLOCKS = 3
EPSILON = 1e-05
WIN = ("win_0", "win_1", "win_2")
LOG2E = math.log2(math.e)
F32 = jnp.float32
BF16 = jnp.bfloat16

NN = (((1,), (0,)), ((), ()))
NT = (((1,), (1,)), ((), ()))


def mm(a, b, dims=NN):
    return lax.dot_general(a, b, dims, preferred_element_type=F32)


def norm(x):
    mean = jnp.sum(x, axis=0, keepdims=True) * (1.0 / C)
    centred = x - mean
    var = jnp.sum(centred * centred, axis=0, keepdims=True) * (1.0 / C)
    return centred, lax.rsqrt(var + EPSILON)


def kernel(
    sizes,
    sigma,
    coords,
    noise,
    single,
    tokens,
    atok,
    wcount,
    pbias,
    tokw,
    gain,
    posw,
    adaw,
    adab,
    attnw,
    outw,
    guw,
    downw,
    finw,
    out,
    s,
):
    ny, nx, nz = sizes
    y, x, z = (lax.axis_index(name) for name in WIN)
    h = lax.axis_index("head")
    other = 1 - h
    slots = coords.shape[1]
    W = slots // 2
    NP = W // 2
    mine = pl.multiple_of(h * W, W)
    theirs = pl.multiple_of(other * W, W)

    me1, me2 = z * 2 + h, y * nx + x

    def wrapped(v, n):
        return jnp.where(v >= n, v - n, v)

    zs = [wrapped(z + d, nz) if d else z for d in range(nz)]
    ys = [wrapped(y + d, ny) if d else y for d in range(ny)]
    xs = [wrapped(x + d, nx) if d else x for d in range(nx)]
    peers1 = [({"win_2": c, "head": a}, c * 2 + a) for c in zs for a in (h, other)][1:]
    peers2 = [({"win_0": c, "win_1": a}, c * nx + a) for c in ys for a in xs][1:]

    count = [0]

    def fetch(src, dst):
        copy = pltpu.make_async_copy(src, dst, s.lsem.at[count[0]])
        count[0] += 1
        copy.start()
        return copy

    small = [
        fetch(coords, s.cfull),
        fetch(noise, s.nfull),
        fetch(wcount, s.wc),
        fetch(sigma, s.sig),
    ]
    prep = [
        fetch(gain, s.rows.at[pl.ds(0, 1)]),
        fetch(posw, s.rows.at[pl.ds(8, 3)]),
        *[fetch(adab.at[b], s.rows.at[pl.ds(16 + 8 * b, 6)]) for b in range(BLOCKS)],
        fetch(finw, s.fin),
        fetch(tokw, s.tokw),
        fetch(tokens.at[pl.ds(pl.multiple_of(h * W * TOKW, W * TOKW), W * TOKW)], s.tok),
    ]
    c_ada = fetch(adaw, s.adaw)
    c_gu = fetch(guw, s.guw)
    c_down = fetch(downw, s.downw)
    own_rows = pl.ds(pl.multiple_of(h * HALF, HALF), HALF)
    own_in = [
        fetch(single.at[pl.ds(mine, W)], s.atoms.at[:, own_rows, :]),
        fetch(atok.at[pl.ds(mine, W)], s.tokidx.at[h]),
        fetch(coords.at[:, pl.ds(mine, W)], s.cpos.at[h]),
        fetch(noise.at[:, pl.ds(mine, W)], s.npos.at[h]),
        fetch(attnw, s.attnT.at[:, :, pl.ds(0, HALF), :]),
        fetch(outw, s.out_l),
        fetch(pbias.at[:, pl.ds(mine, W)], s.bias_l),
    ]

    barrier = pltpu.get_barrier_semaphore()
    for dev, _ in peers1 + peers2:
        pl.semaphore_signal(
            barrier, inc=1, device_id=dev, device_id_type=pl.DeviceIdType.MESH
        )

    lane = lax.broadcasted_iota(jnp.int32, (1, 128), 1)

    for c in small:
        c.wait()
    sig = jnp.broadcast_to(s.sig[...], (1, 128))
    inv = 1.0 / (1.0 + sig * sig)
    root = jnp.sqrt(inv)
    counts = s.wc[...].astype(F32)
    win_id = (y * nx + x) * nz + z
    win_lane = lax.broadcasted_iota(jnp.int32, counts.shape, 1)
    own_count = jnp.sum(jnp.where(win_lane == win_id, counts, 0.0), axis=1, keepdims=True)
    atoms_total = QW * jnp.sum(counts, axis=1, keepdims=True)
    slot = lax.broadcasted_iota(jnp.int32, (slots, HALF), 0).astype(F32)
    live = slot < own_count
    row = jnp.zeros((1, 128), F32)
    for k in range(3):
        noisy = jnp.where(live, s.cfull[k] + sig[:, :HALF] * s.nfull[k], 0.0)
        part = jnp.sum(jnp.sum(noisy, axis=0, keepdims=True), axis=1, keepdims=True)
        row = jnp.where(lane == k, part, row)
    s.red1[me1] = row

    pl.semaphore_wait(barrier, len(peers1) + len(peers2))

    def remote(src, dst, send, recv, dev):
        return pltpu.make_async_remote_copy(
            src_ref=src,
            dst_ref=dst,
            send_sem=send,
            recv_sem=recv,
            device_id=dev,
            device_id_type=pl.DeviceIdType.MESH,
        )

    def spread(buf, me, peers, ssem, rsem):
        sends = []
        for j, (dev, _) in enumerate(peers):
            c = remote(buf.at[me], buf.at[me], ssem.at[j], rsem.at[me], dev)
            c.start()
            sends.append(c)
        return sends

    def collect(buf, peers, ssem, rsem):
        for j, (dev, src) in enumerate(peers):
            remote(buf.at[src], buf.at[src], ssem.at[j], rsem.at[src], dev).wait_recv()

    sends1 = spread(s.red1, me1, peers1, s.ssem1, s.rsem1)

    pair = [0]

    def give(src, dst):
        i = pair[0]
        pair[0] += 1
        c = remote(src, dst, s.psend.at[i], s.precv.at[i], {"head": other})
        c.start()
        return c

    x_atoms = give(single.at[pl.ds(theirs, W)], s.atoms.at[:, own_rows, :])
    x_tok = give(atok.at[pl.ds(theirs, W)], s.tokidx.at[h])
    x_c = give(coords.at[:, pl.ds(theirs, W)], s.cpos.at[h])
    x_n = give(noise.at[:, pl.ds(theirs, W)], s.npos.at[h])
    x_attn = give(attnw, s.attnT.at[:, :, pl.ds(HALF, HALF), :])
    x_out = give(outw, s.out_r)
    x_bias = give(pbias.at[:, pl.ds(theirs, W)], s.bias_r)

    def turned(values, scale=None):
        values = values.T
        if scale is not None:
            values = values * jnp.asarray(scale, BF16)
        return values

    for c in prep:
        c.wait()
    s.tokwT[...] = turned(s.tokw[...])
    columns = s.rows[...].T

    def column(k):
        return jnp.broadcast_to(columns[:, k : k + 1], (C, C))

    s.gainT[...] = column(0)
    for k in range(3):
        s.pwT[k] = column(8 + k)
    for b in range(BLOCKS):
        for j in range(6):
            bias = column(16 + 8 * b + j)
            s.adabT[b * 6 + j] = bias * 0.5 if j in (0, 2, 3, 5) else bias
    c_ada.wait()
    for b in range(BLOCKS):
        for j in range(6):
            s.adaT[b, j * C : (j + 1) * C, :] = turned(
                s.adaw[b, j], 0.5 if j in (0, 2, 3, 5) else None
            )
    s.tpT[...] = mm(s.tokwT[...], s.tok[...], NT).astype(BF16)
    c_gu.wait()
    c_down.wait()
    for b in range(BLOCKS):
        s.guT[b, :HID, :] = turned(s.guw[b, 0], 0.5)
        s.guT[b, HID:, :] = turned(s.guw[b, 1])
        s.downT[b] = turned(s.downw[b], 0.5)

    for c in own_in:
        c.wait()
    for c in (x_tok, x_c, x_n, x_atoms):
        c.wait()
    s.tokcat[...] = jnp.concatenate([s.tokidx[0], s.tokidx[1]], axis=1)
    for k in range(3):
        halves = [(s.cpos[a, k] + sig[:, :HALF] * s.npos[a, k]) * root[:, :HALF] for a in (0, 1)]
        s.pos[k] = jnp.concatenate(halves, axis=1)

    eye = (
        lax.broadcasted_iota(jnp.int32, (C, C), 0) == lax.broadcasted_iota(jnp.int32, (C, C), 1)
    ).astype(BF16)

    def condition(p, at):
        for w in range(2):
            lanes = pl.ds(w * QW, QW)
            win = 2 * p + w
            own = s.tokcat[pl.ds(win, 1), :] + win * TOKW
            ids = lax.broadcasted_iota(jnp.int32, (W * TOKW, QW), 0)
            one_hot = jnp.where(ids == own, 1.0, 0.0).astype(BF16)
            cond = mm(eye, s.atoms[win], NT) + mm(s.tpT[...], one_hot)
            centred, rstd = norm(cond)
            s.cn[at, :, lanes] = (centred * rstd * s.gainT[...]).astype(BF16)
            for k in range(3):
                cond = cond + s.pos[k, pl.ds(win, 1), :] * s.pwT[k]
            s.stream[p, :, lanes] = cond

    def ada_terms(p, at, b):
        terms = mm(s.adaT[b], s.cn[at])
        for j in range(6):
            for w in range(2):
                lanes = pl.ds(w * QW, QW)
                a = terms[j * C : (j + 1) * C, w * QW : (w + 1) * QW] + s.adabT[b * 6 + j]
                if j in (0, 2, 3, 5):
                    a = 1.0 + jnp.tanh(a)
                s.ada[p, b * 6 + j, :, lanes] = a

    def first(step, carry):
        condition(2 * step, 0)
        condition(2 * step + 1, 1)
        for b in range(BLOCKS):
            for at in range(2):
                ada_terms(2 * step + at, at, b)
        return carry

    half = NP // 4
    lax.fori_loop(0, half, first, 0)

    collect(s.red1, peers1, s.ssem1, s.rsem1)
    s.red2[me2] = jnp.sum(s.red1[...], axis=0)
    sends2 = spread(s.red2, me2, peers2, s.ssem2, s.rsem2)

    lax.fori_loop(half, NP // 2, first, 0)

    x_attn.wait()
    x_out.wait()
    for b in range(BLOCKS):
        s.attnT[b, 3] = (s.attnT[b, 3].astype(F32) * 0.5).astype(BF16)
        both = jnp.concatenate([s.out_l[b], s.out_r[b]], axis=0)
        s.outT[b] = turned(both, 0.25)
    x_bias.wait()

    def turn_bias(step, carry):
        for n in range(4):
            w = 4 * step + n
            for a in range(HALF_HEADS):
                for side, buf in enumerate((s.bias_l, s.bias_r)):
                    i = side * HALF_HEADS + a
                    s.biasT[w, :, i * QW : (i + 1) * QW] = buf[a, w].T.astype(F32) * LOG2E
        return carry

    lax.fori_loop(0, W // 4, turn_bias, 0)

    collect(s.red2, peers2, s.ssem2, s.rsem2)
    total = jnp.sum(s.red2[...], axis=0) / atoms_total
    centre = [
        jnp.sum(jnp.where(lane == k, total, 0.0), axis=1, keepdims=True) for k in range(3)
    ]
    shift = jnp.zeros((C, C), F32)
    for k in range(3):
        shift = shift + (centre[k] * root) * s.pwT[k]
    s.shift[...] = shift

    q_scale = LOG2E * HEAD_DIM ** (-0.5)
    quads = NP // 2

    def begin(p, carry):
        for w in range(2):
            lanes = pl.ds(w * QW, QW)
            s.stream[p, :, lanes] = s.stream[p, :, lanes] - s.shift[...]
        return carry

    lax.fori_loop(0, NP, begin, 0)

    def halves(w):
        return slice(w * QW, (w + 1) * QW)

    def place(quad, v):
        return 2 * quad + v // 2, halves(v % 2)

    def project(b, quad, par):
        def normed(v):
            p, lanes = place(quad, v)
            centred, rstd = norm(s.stream[p, :, lanes])
            n = centred * (0.5 * rstd) * s.ada[p, b * 6, :, lanes] + s.ada[p, b * 6 + 1, :, lanes]
            s.n[:, halves(v)] = n.astype(BF16)

        def proj(j0):
          yy = mm(s.attnT[b, j0 : j0 + 2].reshape(2 * C, C), s.n[...])
          for j in (j0, j0 + 1):
            y = yy[(j - j0) * C : (j - j0 + 1) * C]
            if j == 0:
                s.q[par] = (y * q_scale).astype(BF16)
            elif j == 1:
                for v in range(4):
                    s.k[par, v] = y[:, halves(v)].T.astype(BF16)
            elif j == 2:
                s.v[par] = y.astype(BF16)
            else:
                s.gate[par] = 1.0 + jnp.tanh(y)

        return [functools.partial(normed, v) for v in range(4)] + [
            functools.partial(proj, j) for j in (0, 2)
        ]

    def attend(b, quad, par):
        held = {}

        def scores(v):
            cols = []
            for hd in range(HEADS):
                at = hd * HEAD_DIM
                part = [s.q[par, at : at + HEAD_DIM, halves(v)]]
                if at > 0:
                    part = [jnp.zeros((at, QW), BF16)] + part
                if at + HEAD_DIM < C:
                    part = part + [jnp.zeros((C - HEAD_DIM - at, QW), BF16)]
                cols.append(jnp.concatenate(part, axis=0))
            held[v] = mm(s.k[par, v], jnp.concatenate(cols, axis=1))

        def mix(v, hd):
            at = slice(hd * HEAD_DIM, (hd + 1) * HEAD_DIM)
            sc = held[v][:, halves(hd)] + s.biasT[4 * quad + v, :, halves(hd)]
            e = jnp.exp2(sc - jnp.max(sc, axis=0, keepdims=True))
            recip = 1.0 / jnp.sum(e, axis=0, keepdims=True)
            o = mm(s.v[par, at, halves(v)], e.astype(BF16))
            s.att[par, at, halves(v)] = (o * recip * s.gate[par, at, halves(v)]).astype(BF16)

        out = [functools.partial(scores, 0)]
        for v in range(4):
            if v + 1 < 4:
                out.append(functools.partial(scores, v + 1))
            out += [functools.partial(mix, v, hd) for hd in range(HEADS)]
        return out

    def add_attended(b, quad, par):
        held = {}

        def update():
            held[0] = mm(s.outT[b], s.att[par])

        def piece(v):
            p, lanes = place(quad, v)
            xs = s.stream[p, :, lanes] + s.ada[p, b * 6 + 2, :, lanes] * held[0][:, halves(v)]
            s.mid[par, :, halves(v)] = xs
            centred, rstd = norm(xs)
            n = centred * (0.5 * rstd) * s.ada[p, b * 6 + 3, :, lanes]
            s.n2[par, :, halves(v)] = (n + s.ada[p, b * 6 + 4, :, lanes]).astype(BF16)

        return [update] + [functools.partial(piece, v) for v in range(4)]

    def transition(b, quad, par):
        held = {}

        def up(j):
            rows = slice(j * C, (j + 1) * C)
            g = mm(s.guT[b, rows, :], s.n2[par])
            u = mm(s.guT[b, HID + j * C : HID + (j + 1) * C, :], s.n2[par])
            s.hidden[rows, :] = (g * (1.0 + jnp.tanh(g)) * u).astype(BF16)

        def down():
            held[0] = mm(s.downT[b], s.hidden[...])

        def piece(v):
            p, lanes = place(quad, v)
            s.stream[p, :, lanes] = (
                s.mid[par, :, halves(v)] + s.ada[p, b * 6 + 5, :, lanes] * held[0][:, halves(v)]
            )

        return [functools.partial(up, 0), functools.partial(up, 1), down] + [
            functools.partial(piece, v) for v in range(4)
        ]

    steps = (project, attend, add_attended, transition)

    def slot_of(b, t, first_step, last_step):
        work = []
        for n in range(first_step, last_step + 1):
            quad = (t - n) % quads
            block_of = b - (n - t + quads - 1) // quads if n > t else b
            parity = (t - n) % 2
            pieces = steps[n](block_of, quad, parity if n == 0 else parity)
            work.append((n, pieces))
        order = []
        for n, pieces in work:
            for at, piece in enumerate(pieces):
                order.append(((at + 0.5) / len(pieces), -n, piece))
        for _, _, piece in sorted(order, key=lambda entry: entry[:2]):
            piece()

    for t in range(quads):
        slot_of(0, t, 0, min(t, 3))

    def middle(b, carry):
        for t in range(quads):
            slot_of(b, t, 0, 3)
        return carry

    lax.fori_loop(1, BLOCKS, middle, 0)
    for t in range(3):
        slot_of(BLOCKS, t, t + 1, 3)

    final = jnp.concatenate([s.fin[...].astype(F32), jnp.zeros((5, C), F32)], axis=0).astype(BF16)

    def finish(p, carry):
        for w in range(2):
            centred, rstd = norm(s.stream[p, :, pl.ds(w * QW, QW)])
            upd = mm(final, (centred * rstd).astype(BF16))
            for k in range(3):
                s.upd[k, pl.ds(2 * p + w, 1), :] = upd[k : k + 1, :]
        return carry

    lax.fori_loop(0, NP, finish, 0)
    x_upd = give(s.upd, s.updr)

    def write(source, first_slot):
        first_slot = pl.multiple_of(first_slot, W)
        ids = (lax.broadcasted_iota(jnp.int32, (W, HALF), 0) + first_slot).astype(F32)
        alive = ids < own_count
        for k in range(3):
            both = source[k]
            upd = jnp.where(h == 0, both[:, :HALF], both[:, HALF:])
            here = pl.ds(first_slot, W)
            noisy = s.cfull[k, here, :] + sig[:, :HALF] * s.nfull[k, here, :]
            shifted = noisy - centre[k]
            value = shifted * inv[:, :HALF] + (sig * root)[:, :HALF] * upd
            out[k, here, :] = jnp.where(alive, value, 0.0)

    write(s.upd, mine)
    x_upd.wait()
    write(s.updr, theirs)
    for c in sends1 + sends2:
        c.wait_send()


class Scratch:
    pass


def scratch_of(slots, nz, nxy):
    win_total = nz * nxy
    W = slots // 2
    NP = W // 2
    V = pltpu.VMEM
    return {
        "cfull": V((3, slots, HALF), F32),
        "nfull": V((3, slots, HALF), F32),
        "wc": V((1, win_total), jnp.int32),
        "sig": V((1, 1), F32),
        "rows": V((C, C), F32),
        "fin": V((3, C), BF16),
        "tokw": V((3 * C, C), BF16),
        "tok": V((W * TOKW, 3 * C), BF16),
        "adaw": V((BLOCKS, 6, C, C), BF16),
        "guw": V((BLOCKS, 2, C, HID), BF16),
        "downw": V((BLOCKS, HID, C), BF16),
        "atoms": V((W, QW, C), BF16),
        "tokidx": V((2, W, HALF), jnp.int32),
        "cpos": V((2, 3, W, HALF), F32),
        "npos": V((2, 3, W, HALF), F32),
        "out_l": V((BLOCKS, HALF, C), BF16),
        "out_r": V((BLOCKS, HALF, C), BF16),
        "bias_l": V((2, W, QW, QW), BF16),
        "bias_r": V((2, W, QW, QW), BF16),
        "red1": V((2 * nz, 1, 128), F32),
        "red2": V((nxy, 1, 128), F32),
        "tokwT": V((C, 3 * C), BF16),
        "gainT": V((C, C), F32),
        "pwT": V((3, C, C), F32),
        "adabT": V((BLOCKS * 6, C, C), F32),
        "adaT": V((BLOCKS, 6 * C, C), BF16),
        "attnT": V((BLOCKS, 4, C, C), BF16),
        "outT": V((BLOCKS, C, C), BF16),
        "guT": V((BLOCKS, 2 * HID, C), BF16),
        "downT": V((BLOCKS, C, HID), BF16),
        "tpT": V((C, W * TOKW), BF16),
        "tokcat": V((W, QW), jnp.int32),
        "pos": V((3, W, QW), F32),
        "cn": V((2, C, 2 * QW), BF16),
        "stream": V((NP, C, 2 * QW), F32),
        "ada": V((NP, BLOCKS * 6, C, 2 * QW), F32),
        "biasT": V((W, QW, HEADS * QW), F32),
        "shift": V((C, C), F32),
        "n": V((C, 4 * QW), BF16),
        "q": V((2, C, 4 * QW), BF16),
        "k": V((2, 4, QW, C), BF16),
        "v": V((2, C, 4 * QW), BF16),
        "gate": V((2, C, 4 * QW), F32),
        "att": V((2, C, 4 * QW), BF16),
        "mid": V((2, C, 4 * QW), F32),
        "n2": V((2, C, 4 * QW), BF16),
        "hidden": V((HID, 4 * QW), BF16),
        "upd": V((3, W, QW), F32),
        "updr": V((3, W, QW), F32),
        "lsem": pltpu.SemaphoreType.DMA((24,)),
        "ssem1": pltpu.SemaphoreType.DMA((2 * nz,)),
        "rsem1": pltpu.SemaphoreType.DMA((2 * nz,)),
        "ssem2": pltpu.SemaphoreType.DMA((nxy,)),
        "rsem2": pltpu.SemaphoreType.DMA((nxy,)),
        "psend": pltpu.SemaphoreType.DMA((8,)),
        "precv": pltpu.SemaphoreType.DMA((8,)),
    }


def make_local(sizes):
    def local(
        coords,
        noise,
        sigma,
        atom_single,
        token_single,
        atom_token,
        window_count,
        pair_bias,
        token_weight,
        cond_gain,
        position_weight,
        ada_weight,
        ada_bias,
        attn_weight,
        out_weight,
        gateup_weight,
        down_weight,
        final_weight,
    ):
        slots = coords.shape[1]
        ny, nx, nz = sizes
        scratch = scratch_of(slots, nz, ny * nx)
        names = list(scratch)

        def body(*refs):
            s = Scratch()
            for name, ref in zip(names, refs[19:]):
                setattr(s, name, ref)
            kernel(sizes, *refs[:19], s)

        any_spec = pl.BlockSpec(memory_space=pl.ANY)
        return pl.pallas_call(
            body,
            out_shape=jax.ShapeDtypeStruct(coords.shape, F32),
            in_specs=[any_spec] * 18,
            out_specs=pl.BlockSpec(memory_space=pltpu.VMEM),
            scratch_shapes=[scratch[name] for name in names],
            compiler_params=pltpu.CompilerParams(
                collective_id=0, has_side_effects=True, vmem_limit_bytes=60 * 1024 * 1024
            ),
            name="denoise",
        )(
            sigma.reshape(1, 1),
            coords,
            noise,
            atom_single,
            token_single,
            atom_token,
            window_count.reshape(1, -1),
            pair_bias,
            token_weight,
            cond_gain.reshape(1, -1),
            position_weight,
            ada_weight,
            ada_bias,
            jnp.swapaxes(attn_weight, 2, 3),
            out_weight,
            gateup_weight,
            down_weight,
            final_weight,
        )

    return local


def solution(mesh):
    devices = mesh.devices
    head = mesh.shape["head"]
    sizes = (4, 4, 8) if devices.size == 256 else (2, 2, devices.size // (4 * head))
    torus = Mesh(devices.reshape(*sizes, head), WIN + ("head",))
    in_specs = (
        P(None, WIN, "head"),
        P(None, WIN, "head"),
        P(),
        P(WIN, "head", None),
        P(WIN, None),
        P(WIN, "head"),
        P(),
        P("head", WIN, None, None),
        P(),
        P(),
        P(),
        P(),
        P(),
        P(None, None, None, "head"),
        P(None, "head", None),
        P(),
        P(),
        P(),
    )
    out_specs = P(None, WIN, "head")
    return jax.shard_map(
        make_local(sizes), mesh=torus, in_specs=in_specs, out_specs=out_specs, check_vma=False
    )
```

```python
import functools
import math

import jax
import jax.numpy as jnp
from jax import lax
from jax.experimental import pallas as pl
from jax.experimental.pallas import tpu as pltpu
from jax.sharding import Mesh
from jax.sharding import PartitionSpec as P

HEADS = 4
HEAD_DIM = 32
HALF_HEADS = 2
C = 128
QW = 128
HALF = 64
HID = 256
TOKW = 16
BLOCKS = 3
EPSILON = 1e-05
WIN = ("win_0", "win_1", "win_2")
LOG2E = math.log2(math.e)
F32 = jnp.float32
BF16 = jnp.bfloat16

NN = (((1,), (0,)), ((), ()))
NT = (((1,), (1,)), ((), ()))


def mm(a, b, dims=NN):
    return lax.dot_general(a, b, dims, preferred_element_type=F32)


def norm(x):
    mean = jnp.sum(x, axis=0, keepdims=True) * (1.0 / C)
    centred = x - mean
    var = jnp.sum(centred * centred, axis=0, keepdims=True) * (1.0 / C)
    return centred, lax.rsqrt(var + EPSILON)


def kernel(
    sizes,
    sigma,
    coords,
    noise,
    single,
    tokens,
    atok,
    wcount,
    pbias,
    tokw,
    gain,
    posw,
    adaw,
    adab,
    attnw,
    outw,
    guw,
    downw,
    finw,
    out,
    s,
):
    ny, nx, nz = sizes
    y, x, z = (lax.axis_index(name) for name in WIN)
    h = lax.axis_index("head")
    other = 1 - h
    slots = coords.shape[1]
    W = slots // 2
    NP = W // 2
    mine = pl.multiple_of(h * W, W)
    theirs = pl.multiple_of(other * W, W)

    me1, me2 = z * 2 + h, y * nx + x

    def wrapped(v, n):
        return jnp.where(v >= n, v - n, v)

    zs = [wrapped(z + d, nz) if d else z for d in range(nz)]
    ys = [wrapped(y + d, ny) if d else y for d in range(ny)]
    xs = [wrapped(x + d, nx) if d else x for d in range(nx)]
    peers1 = [({"win_2": c, "head": a}, c * 2 + a) for c in zs for a in (h, other)][1:]
    peers2 = [({"win_0": c, "win_1": a}, c * nx + a) for c in ys for a in xs][1:]

    count = [0]

    def fetch(src, dst):
        copy = pltpu.make_async_copy(src, dst, s.lsem.at[count[0]])
        count[0] += 1
        copy.start()
        return copy

    small = [
        fetch(coords, s.cfull),
        fetch(noise, s.nfull),
        fetch(wcount, s.wc),
        fetch(sigma, s.sig),
    ]
    prep = [
        fetch(gain, s.rows.at[pl.ds(0, 1)]),
        fetch(posw, s.rows.at[pl.ds(8, 3)]),
        *[fetch(adab.at[b], s.rows.at[pl.ds(16 + 8 * b, 6)]) for b in range(BLOCKS)],
        fetch(finw, s.fin),
        fetch(tokw, s.tokw),
        fetch(tokens.at[pl.ds(pl.multiple_of(h * W * TOKW, W * TOKW), W * TOKW)], s.tok),
    ]
    c_ada = fetch(adaw, s.adaw)
    c_gu = fetch(guw, s.guw)
    c_down = fetch(downw, s.downw)
    own_rows = pl.ds(pl.multiple_of(h * HALF, HALF), HALF)
    own_in = [
        fetch(single.at[pl.ds(mine, W)], s.atoms.at[:, own_rows, :]),
        fetch(atok.at[pl.ds(mine, W)], s.tokidx.at[h]),
        fetch(coords.at[:, pl.ds(mine, W)], s.cpos.at[h]),
        fetch(noise.at[:, pl.ds(mine, W)], s.npos.at[h]),
        fetch(attnw, s.attnT.at[:, :, pl.ds(0, HALF), :]),
        fetch(outw, s.out_l),
        fetch(pbias.at[:, pl.ds(mine, W)], s.bias_l),
    ]

    barrier = pltpu.get_barrier_semaphore()
    for dev, _ in peers1 + peers2:
        pl.semaphore_signal(
            barrier, inc=1, device_id=dev, device_id_type=pl.DeviceIdType.MESH
        )

    lane = lax.broadcasted_iota(jnp.int32, (1, 128), 1)

    for c in small:
        c.wait()
    sig = jnp.broadcast_to(s.sig[...], (1, 128))
    inv = 1.0 / (1.0 + sig * sig)
    root = jnp.sqrt(inv)
    counts = s.wc[...].astype(F32)
    win_id = (y * nx + x) * nz + z
    win_lane = lax.broadcasted_iota(jnp.int32, counts.shape, 1)
    own_count = jnp.sum(jnp.where(win_lane == win_id, counts, 0.0), axis=1, keepdims=True)
    atoms_total = QW * jnp.sum(counts, axis=1, keepdims=True)
    slot = lax.broadcasted_iota(jnp.int32, (slots, HALF), 0).astype(F32)
    live = slot < own_count
    row = jnp.zeros((1, 128), F32)
    for k in range(3):
        noisy = jnp.where(live, s.cfull[k] + sig[:, :HALF] * s.nfull[k], 0.0)
        part = jnp.sum(jnp.sum(noisy, axis=0, keepdims=True), axis=1, keepdims=True)
        row = jnp.where(lane == k, part, row)
    s.red1[me1] = row

    pl.semaphore_wait(barrier, len(peers1) + len(peers2))

    def remote(src, dst, send, recv, dev):
        return pltpu.make_async_remote_copy(
            src_ref=src,
            dst_ref=dst,
            send_sem=send,
            recv_sem=recv,
            device_id=dev,
            device_id_type=pl.DeviceIdType.MESH,
        )

    def spread(buf, me, peers, ssem, rsem):
        sends = []
        for j, (dev, _) in enumerate(peers):
            c = remote(buf.at[me], buf.at[me], ssem.at[j], rsem.at[me], dev)
            c.start()
            sends.append(c)
        return sends

    def collect(buf, peers, ssem, rsem):
        for j, (dev, src) in enumerate(peers):
            remote(buf.at[src], buf.at[src], ssem.at[j], rsem.at[src], dev).wait_recv()

    sends1 = spread(s.red1, me1, peers1, s.ssem1, s.rsem1)

    pair = [0]

    def give(src, dst):
        i = pair[0]
        pair[0] += 1
        c = remote(src, dst, s.psend.at[i], s.precv.at[i], {"head": other})
        c.start()
        return c

    x_atoms = give(single.at[pl.ds(theirs, W)], s.atoms.at[:, own_rows, :])
    x_tok = give(atok.at[pl.ds(theirs, W)], s.tokidx.at[h])
    x_c = give(coords.at[:, pl.ds(theirs, W)], s.cpos.at[h])
    x_n = give(noise.at[:, pl.ds(theirs, W)], s.npos.at[h])
    x_attn = give(attnw, s.attnT.at[:, :, pl.ds(HALF, HALF), :])
    x_out = give(outw, s.out_r)
    x_bias = give(pbias.at[:, pl.ds(theirs, W)], s.bias_r)

    def turned(values, scale=None):
        values = values.T
        if scale is not None:
            values = values * jnp.asarray(scale, BF16)
        return values

    for c in prep:
        c.wait()
    s.tokwT[...] = turned(s.tokw[...])
    columns = s.rows[...].T

    def column(k):
        return jnp.broadcast_to(columns[:, k : k + 1], (C, C))

    s.gainT[...] = column(0)
    for k in range(3):
        s.pwT[k] = column(8 + k)
    for b in range(BLOCKS):
        for j in range(6):
            bias = column(16 + 8 * b + j)
            s.adabT[b * 6 + j] = bias * 0.5 if j in (0, 2, 3, 5) else bias
    c_ada.wait()
    for b in range(BLOCKS):
        for j in range(6):
            s.adaT[b, j * C : (j + 1) * C, :] = turned(
                s.adaw[b, j], 0.5 if j in (0, 2, 3, 5) else None
            )
    s.tpT[...] = mm(s.tokwT[...], s.tok[...], NT).astype(BF16)
    c_gu.wait()
    c_down.wait()
    for b in range(BLOCKS):
        s.guT[b, :HID, :] = turned(s.guw[b, 0], 0.5)
        s.guT[b, HID:, :] = turned(s.guw[b, 1])
        s.downT[b] = turned(s.downw[b], 0.5)

    for c in own_in:
        c.wait()
    for c in (x_tok, x_c, x_n, x_atoms):
        c.wait()
    s.tokcat[...] = jnp.concatenate([s.tokidx[0], s.tokidx[1]], axis=1)
    for k in range(3):
        halves = [(s.cpos[a, k] + sig[:, :HALF] * s.npos[a, k]) * root[:, :HALF] for a in (0, 1)]
        s.pos[k] = jnp.concatenate(halves, axis=1)

    eye = (
        lax.broadcasted_iota(jnp.int32, (C, C), 0) == lax.broadcasted_iota(jnp.int32, (C, C), 1)
    ).astype(BF16)

    def condition(p, at):
        for w in range(2):
            lanes = pl.ds(w * QW, QW)
            win = 2 * p + w
            own = s.tokcat[pl.ds(win, 1), :] + win * TOKW
            ids = lax.broadcasted_iota(jnp.int32, (W * TOKW, QW), 0)
            one_hot = jnp.where(ids == own, 1.0, 0.0).astype(BF16)
            cond = mm(eye, s.atoms[win], NT) + mm(s.tpT[...], one_hot)
            centred, rstd = norm(cond)
            s.cn[at, :, lanes] = (centred * rstd * s.gainT[...]).astype(BF16)
            for k in range(3):
                cond = cond + s.pos[k, pl.ds(win, 1), :] * s.pwT[k]
            s.stream[p, :, lanes] = cond

    def ada_terms(p, at, b):
        terms = mm(s.adaT[b], s.cn[at])
        for j in range(6):
            for w in range(2):
                lanes = pl.ds(w * QW, QW)
                a = terms[j * C : (j + 1) * C, w * QW : (w + 1) * QW] + s.adabT[b * 6 + j]
                if j in (0, 2, 3, 5):
                    a = 1.0 + jnp.tanh(a)
                s.ada[p, b * 6 + j, :, lanes] = a

    def first(step, carry):
        condition(2 * step, 0)
        condition(2 * step + 1, 1)
        for b in range(BLOCKS):
            for at in range(2):
                ada_terms(2 * step + at, at, b)
        return carry

    half = NP // 4
    lax.fori_loop(0, half, first, 0)

    collect(s.red1, peers1, s.ssem1, s.rsem1)
    s.red2[me2] = jnp.sum(s.red1[...], axis=0)
    sends2 = spread(s.red2, me2, peers2, s.ssem2, s.rsem2)

    lax.fori_loop(half, NP // 2, first, 0)

    x_attn.wait()
    x_out.wait()
    for b in range(BLOCKS):
        s.attnT[b, 3] = (s.attnT[b, 3].astype(F32) * 0.5).astype(BF16)
        both = jnp.concatenate([s.out_l[b], s.out_r[b]], axis=0)
        s.outT[b] = turned(both, 0.25)
    x_bias.wait()

    def turn_bias(step, carry):
        for n in range(4):
            w = 4 * step + n
            for a in range(HALF_HEADS):
                for side, buf in enumerate((s.bias_l, s.bias_r)):
                    i = side * HALF_HEADS + a
                    s.biasT[w, :, i * QW : (i + 1) * QW] = buf[a, w].T.astype(F32) * LOG2E
        return carry

    lax.fori_loop(0, W // 4, turn_bias, 0)

    collect(s.red2, peers2, s.ssem2, s.rsem2)
    total = jnp.sum(s.red2[...], axis=0) / atoms_total
    centre = [
        jnp.sum(jnp.where(lane == k, total, 0.0), axis=1, keepdims=True) for k in range(3)
    ]
    shift = jnp.zeros((C, C), F32)
    for k in range(3):
        shift = shift + (centre[k] * root) * s.pwT[k]
    s.shift[...] = shift

    q_scale = LOG2E * HEAD_DIM ** (-0.5)
    quads = NP // 2

    def begin(p, carry):
        for w in range(2):
            lanes = pl.ds(w * QW, QW)
            s.stream[p, :, lanes] = s.stream[p, :, lanes] - s.shift[...]
        return carry

    lax.fori_loop(0, NP, begin, 0)

    def halves(w):
        return slice(w * QW, (w + 1) * QW)

    def place(quad, v):
        return 2 * quad + v // 2, halves(v % 2)

    def project(b, quad, par):
        def normed(v):
            p, lanes = place(quad, v)
            centred, rstd = norm(s.stream[p, :, lanes])
            n = centred * (0.5 * rstd) * s.ada[p, b * 6, :, lanes] + s.ada[p, b * 6 + 1, :, lanes]
            s.n[:, halves(v)] = n.astype(BF16)

        def proj(j0):
          yy = mm(s.attnT[b, j0 : j0 + 2].reshape(2 * C, C), s.n[...])
          for j in (j0, j0 + 1):
            y = yy[(j - j0) * C : (j - j0 + 1) * C]
            if j == 0:
                s.q[par] = (y * q_scale).astype(BF16)
            elif j == 1:
                for v in range(4):
                    s.k[par, v] = y[:, halves(v)].T.astype(BF16)
            elif j == 2:
                s.v[par] = y.astype(BF16)
            else:
                s.gate[par] = 1.0 + jnp.tanh(y)

        return [functools.partial(normed, v) for v in range(4)] + [
            functools.partial(proj, j) for j in (0, 2)
        ]

    def attend(b, quad, par):
        held = {}

        def scores(v):
            cols = []
            for hd in range(HEADS):
                at = hd * HEAD_DIM
                part = [s.q[par, at : at + HEAD_DIM, halves(v)]]
                if at > 0:
                    part = [jnp.zeros((at, QW), BF16)] + part
                if at + HEAD_DIM < C:
                    part = part + [jnp.zeros((C - HEAD_DIM - at, QW), BF16)]
                cols.append(jnp.concatenate(part, axis=0))
            held[v] = mm(s.k[par, v], jnp.concatenate(cols, axis=1))

        def mix(v, hd):
            at = slice(hd * HEAD_DIM, (hd + 1) * HEAD_DIM)
            sc = held[v][:, halves(hd)] + s.biasT[4 * quad + v, :, halves(hd)]
            e = jnp.exp2(sc - jnp.max(sc, axis=0, keepdims=True))
            recip = 1.0 / jnp.sum(e, axis=0, keepdims=True)
            held[v, hd] = (mm(s.v[par, at, halves(v)], e.astype(BF16)), recip)

        def close(v, hd):
            at = slice(hd * HEAD_DIM, (hd + 1) * HEAD_DIM)
            o, recip = held.pop((v, hd))
            s.att[par, at, halves(v)] = (o * recip * s.gate[par, at, halves(v)]).astype(BF16)

        units = [(v, hd) for v in range(4) for hd in range(HEADS)]
        out = [functools.partial(scores, v) for v in range(2)]
        for n, (v, hd) in enumerate(units):
            if hd == 0 and v + 2 < 4:
                out.append(functools.partial(scores, v + 2))
            out.append(functools.partial(mix, v, hd))
            if n >= 1:
                out.append(functools.partial(close, *units[n - 1]))
        return out + [functools.partial(close, *unit) for unit in units[-1:]]

    def add_attended(b, quad, par):
        def update():
            u = mm(s.outT[b], s.att[par])
            for v in range(4):
                p, lanes = place(quad, v)
                s.mid[par, :, halves(v)] = (
                    s.stream[p, :, lanes] + s.ada[p, b * 6 + 2, :, lanes] * u[:, halves(v)]
                )

        def piece(v):
            p, lanes = place(quad, v)
            centred, rstd = norm(s.mid[par, :, halves(v)])
            n = centred * (0.5 * rstd) * s.ada[p, b * 6 + 3, :, lanes]
            s.n2[par, :, halves(v)] = (n + s.ada[p, b * 6 + 4, :, lanes]).astype(BF16)

        return [update] + [functools.partial(piece, v) for v in range(4)]

    def transition(b, quad, par):
        def up(j):
            rows = slice(j * C, (j + 1) * C)
            g = mm(s.guT[b, rows, :], s.n2[par])
            u = mm(s.guT[b, HID + j * C : HID + (j + 1) * C, :], s.n2[par])
            s.hidden[rows, :] = (g * (1.0 + jnp.tanh(g)) * u).astype(BF16)

        def down():
            d = mm(s.downT[b], s.hidden[...])
            for v in range(4):
                p, lanes = place(quad, v)
                s.stream[p, :, lanes] = (
                    s.mid[par, :, halves(v)] + s.ada[p, b * 6 + 5, :, lanes] * d[:, halves(v)]
                )

        return [functools.partial(up, 0), functools.partial(up, 1), down]

    steps = (project, attend, add_attended, transition)

    def slot_of(b, t, first_step, last_step):
        work = []
        for n in range(first_step, last_step + 1):
            quad = (t - n) % quads
            block_of = b - (n - t + quads - 1) // quads if n > t else b
            parity = (t - n) % 2
            pieces = steps[n](block_of, quad, parity if n == 0 else parity)
            work.append((n, pieces))
        order = []
        for n, pieces in work:
            for at, piece in enumerate(pieces):
                order.append(((at + 0.5) / len(pieces), -n, piece))
        for _, _, piece in sorted(order, key=lambda entry: entry[:2]):
            piece()

    for t in range(quads):
        slot_of(0, t, 0, min(t, 3))

    def middle(b, carry):
        for t in range(quads):
            slot_of(b, t, 0, 3)
        return carry

    lax.fori_loop(1, BLOCKS, middle, 0)
    for t in range(3):
        slot_of(BLOCKS, t, t + 1, 3)

    final = jnp.concatenate([s.fin[...].astype(F32), jnp.zeros((5, C), F32)], axis=0).astype(BF16)

    def finish(quad, carry):
        for v in range(4):
            p, lanes = place(quad, v)
            centred, rstd = norm(s.stream[p, :, lanes])
            upd = mm(final, (centred * rstd).astype(BF16))
            for k in range(3):
                s.upd[k, pl.ds(4 * quad + v, 1), :] = upd[k : k + 1, :]
        return carry

    lax.fori_loop(0, quads, finish, 0)
    x_upd = give(s.upd, s.updr)

    def write(source, first_slot):
        first_slot = pl.multiple_of(first_slot, W)
        ids = (lax.broadcasted_iota(jnp.int32, (W, HALF), 0) + first_slot).astype(F32)
        alive = ids < own_count
        for k in range(3):
            both = source[k]
            upd = jnp.where(h == 0, both[:, :HALF], both[:, HALF:])
            here = pl.ds(first_slot, W)
            noisy = s.cfull[k, here, :] + sig[:, :HALF] * s.nfull[k, here, :]
            shifted = noisy - centre[k]
            value = shifted * inv[:, :HALF] + (sig * root)[:, :HALF] * upd
            out[k, here, :] = jnp.where(alive, value, 0.0)

    write(s.upd, mine)
    x_upd.wait()
    write(s.updr, theirs)
    for c in sends1 + sends2:
        c.wait_send()


class Scratch:
    pass


def scratch_of(slots, nz, nxy):
    win_total = nz * nxy
    W = slots // 2
    NP = W // 2
    V = pltpu.VMEM
    return {
        "cfull": V((3, slots, HALF), F32),
        "nfull": V((3, slots, HALF), F32),
        "wc": V((1, win_total), jnp.int32),
        "sig": V((1, 1), F32),
        "rows": V((C, C), F32),
        "fin": V((3, C), BF16),
        "tokw": V((3 * C, C), BF16),
        "tok": V((W * TOKW, 3 * C), BF16),
        "adaw": V((BLOCKS, 6, C, C), BF16),
        "guw": V((BLOCKS, 2, C, HID), BF16),
        "downw": V((BLOCKS, HID, C), BF16),
        "atoms": V((W, QW, C), BF16),
        "tokidx": V((2, W, HALF), jnp.int32),
        "cpos": V((2, 3, W, HALF), F32),
        "npos": V((2, 3, W, HALF), F32),
        "out_l": V((BLOCKS, HALF, C), BF16),
        "out_r": V((BLOCKS, HALF, C), BF16),
        "bias_l": V((2, W, QW, QW), BF16),
        "bias_r": V((2, W, QW, QW), BF16),
        "red1": V((2 * nz, 1, 128), F32),
        "red2": V((nxy, 1, 128), F32),
        "tokwT": V((C, 3 * C), BF16),
        "gainT": V((C, C), F32),
        "pwT": V((3, C, C), F32),
        "adabT": V((BLOCKS * 6, C, C), F32),
        "adaT": V((BLOCKS, 6 * C, C), BF16),
        "attnT": V((BLOCKS, 4, C, C), BF16),
        "outT": V((BLOCKS, C, C), BF16),
        "guT": V((BLOCKS, 2 * HID, C), BF16),
        "downT": V((BLOCKS, C, HID), BF16),
        "tpT": V((C, W * TOKW), BF16),
        "tokcat": V((W, QW), jnp.int32),
        "pos": V((3, W, QW), F32),
        "cn": V((2, C, 2 * QW), BF16),
        "stream": V((NP, C, 2 * QW), F32),
        "ada": V((NP, BLOCKS * 6, C, 2 * QW), F32),
        "biasT": V((W, QW, HEADS * QW), F32),
        "shift": V((C, C), F32),
        "n": V((C, 4 * QW), BF16),
        "q": V((2, C, 4 * QW), BF16),
        "k": V((2, 4, QW, C), BF16),
        "v": V((2, C, 4 * QW), BF16),
        "gate": V((2, C, 4 * QW), F32),
        "att": V((2, C, 4 * QW), BF16),
        "mid": V((2, C, 4 * QW), F32),
        "n2": V((2, C, 4 * QW), BF16),
        "hidden": V((HID, 4 * QW), BF16),
        "upd": V((3, W, QW), F32),
        "updr": V((3, W, QW), F32),
        "lsem": pltpu.SemaphoreType.DMA((24,)),
        "ssem1": pltpu.SemaphoreType.DMA((2 * nz,)),
        "rsem1": pltpu.SemaphoreType.DMA((2 * nz,)),
        "ssem2": pltpu.SemaphoreType.DMA((nxy,)),
        "rsem2": pltpu.SemaphoreType.DMA((nxy,)),
        "psend": pltpu.SemaphoreType.DMA((8,)),
        "precv": pltpu.SemaphoreType.DMA((8,)),
    }


def make_local(sizes):
    def local(
        coords,
        noise,
        sigma,
        atom_single,
        token_single,
        atom_token,
        window_count,
        pair_bias,
        token_weight,
        cond_gain,
        position_weight,
        ada_weight,
        ada_bias,
        attn_weight,
        out_weight,
        gateup_weight,
        down_weight,
        final_weight,
    ):
        slots = coords.shape[1]
        ny, nx, nz = sizes
        scratch = scratch_of(slots, nz, ny * nx)
        names = list(scratch)

        def body(*refs):
            s = Scratch()
            for name, ref in zip(names, refs[19:]):
                setattr(s, name, ref)
            kernel(sizes, *refs[:19], s)

        any_spec = pl.BlockSpec(memory_space=pl.ANY)
        return pl.pallas_call(
            body,
            out_shape=pltpu.VMEM(coords.shape, F32),
            in_specs=[any_spec] * 18,
            out_specs=pl.BlockSpec(memory_space=pltpu.VMEM),
            scratch_shapes=[scratch[name] for name in names],
            compiler_params=pltpu.CompilerParams(
                collective_id=0, has_side_effects=True, vmem_limit_bytes=56 * 1024 * 1024
            ),
            name="denoise",
        )(
            sigma.reshape(1, 1),
            coords,
            noise,
            atom_single,
            token_single,
            atom_token,
            window_count.reshape(1, -1),
            pair_bias,
            token_weight,
            cond_gain.reshape(1, -1),
            position_weight,
            ada_weight,
            ada_bias,
            jnp.swapaxes(attn_weight, 2, 3),
            out_weight,
            gateup_weight,
            down_weight,
            final_weight,
        )

    return local


def solution(mesh):
    devices = mesh.devices
    head = mesh.shape["head"]
    sizes = (4, 4, 8) if devices.size == 256 else (2, 2, devices.size // (4 * head))
    torus = Mesh(devices.reshape(*sizes, head), WIN + ("head",))
    in_specs = (
        P(None, WIN, "head"),
        P(None, WIN, "head"),
        P(),
        P(WIN, "head", None),
        P(WIN, None),
        P(WIN, "head"),
        P(),
        P("head", WIN, None, None),
        P(),
        P(),
        P(),
        P(),
        P(),
        P(None, None, None, "head"),
        P(None, "head", None),
        P(),
        P(),
        P(),
    )
    out_specs = P(None, WIN, "head")
    return jax.shard_map(
        make_local(sizes), mesh=torus, in_specs=in_specs, out_specs=out_specs, check_vma=False
    )
```
